16 devices in a mesh: pc: 4 (over z, y), pr: 4 (over x, core).
Axes of the slice: x: 2, y: 2, z: 2, core: 2. Of those that a mesh axis runs over, the one named last changes fastest.
Arguments:
- panel_in: float32 [12288, 16, 256], P('pr', 'pc')
- trail_in: float32 [12288, 8192], P('pr', 'pc')
Outputs:
- output 1: float32 [12288, 16, 256], P('pr', 'pc')
- output 2: float32 [12288, 8192], P('pr', 'pc')
All inputs are finite; a program needn't handle non-finite values.
Results may differ from the reference program's by a relative error of at most 0.001.
Values sent between devices are 32-bit elements.
A program may use at most 1 GiB of HBM per device.

```python
import jax
import jax.numpy as jnp
from jax import lax

N = 12288
NB = 256
K = 16
PR = 4
PC = 4
RANK = 2048

BLOCKS = N // NB
ROW_BLOCKS = BLOCKS // PR
TRAIL_COLS = N - K * NB
PREC_HIGH = lax.Precision.HIGHEST


def rows_to_owner(full_mat):
    col_width = full_mat.shape[1]
    return full_mat.reshape(ROW_BLOCKS, PR, NB, col_width).transpose(1, 0, 2, 3).reshape(N, col_width)


def rows_from_owner(stored):
    col_width = stored.shape[1]
    return stored.reshape(PR, ROW_BLOCKS, NB, col_width).transpose(1, 0, 2, 3).reshape(N, col_width)


def cols_to_owner(full_mat):
    block_count = full_mat.shape[1] // NB
    return full_mat.reshape(N, block_count // PC, PC, NB).transpose(0, 2, 1, 3).reshape(N, block_count, NB)


def cols_from_owner(stored):
    block_count = stored.shape[1]
    return stored.reshape(N, PC, block_count // PC, NB).transpose(0, 2, 1, 3).reshape(N, block_count * NB)


def build_layout(full_mat):
    row_major = rows_to_owner(full_mat)
    panel_in = cols_to_owner(row_major[:, :K * NB])
    trail_in = cols_to_owner(row_major[:, K * NB:]).reshape(N, TRAIL_COLS)
    return {"panel_in": panel_in, "trail_in": trail_in}


def setup_inputs(seed: int = 0) -> dict:
    key_low, key_diag = jax.random.split(jax.random.key(seed))
    factor = jax.random.normal(key_low, (N, RANK), jnp.float32)
    diag_shift = 0.5 + jax.random.uniform(key_diag, (N,), jnp.float32)
    low_rank = jnp.dot(factor, factor.T, precision=PREC_HIGH) / RANK
    full_mat = 0.5 * (low_rank + low_rank.T) + jnp.diag(diag_shift)
    return build_layout(full_mat)


def reference(panel_in, trail_in):
    stored = jnp.concatenate([cols_from_owner(panel_in), cols_from_owner(trail_in.reshape(N, BLOCKS - K, NB))], axis=1)
    work_mat = rows_from_owner(stored)
    factor_cols = []
    kept_rows = []
    for panel_step in range(K):
        l_diag = jnp.linalg.cholesky(work_mat[:NB, :NB])
        below_diag = lax.linalg.triangular_solve(l_diag, work_mat[NB:, :NB], left_side=False, lower=True, transpose_a=True)
        factor_cols.append(jnp.concatenate([jnp.zeros((panel_step * NB, NB), work_mat.dtype), l_diag, below_diag], axis=0))
        kept_rows.append(work_mat[:NB, (K - panel_step) * NB:])
        work_mat = work_mat[NB:, NB:] - jnp.dot(below_diag, below_diag.T, precision=PREC_HIGH)
    panel_full = jnp.concatenate(factor_cols, axis=1)
    trail_full = jnp.concatenate(kept_rows + [work_mat], axis=0)
    panel_out = cols_to_owner(rows_to_owner(panel_full))
    trail_out = cols_to_owner(rows_to_owner(trail_full)).reshape(N, TRAIL_COLS)
    return panel_out, trail_out
```

```python
import functools

import jax
import jax.numpy as jnp
from jax import lax
from jax.experimental import pallas as pl
from jax.experimental.pallas import tpu as pltpu
from jax.sharding import PartitionSpec as P


F32 = jnp.float32
BF16 = jnp.bfloat16
HIGH = lax.Precision.HIGHEST
NB = 256
SUP = 1024
VMEM_LIMIT = 60 * 1024 * 1024


def dot(a, b):
    return lax.dot_general(a, b, (((1,), (0,)), ((), ())), precision=HIGH, preferred_element_type=F32)


def dot_nt(a, b):
    return lax.dot_general(a, b, (((1,), (1,)), ((), ())), precision=HIGH, preferred_element_type=F32)


def dot_tn(a, b):
    return lax.dot_general(a, b, (((0,), (0,)), ((), ())), precision=HIGH, preferred_element_type=F32)


def split3(x):
    high = x.astype(BF16)
    rest = x - high.astype(F32)
    mid = rest.astype(BF16)
    return high, mid, (rest - mid.astype(F32)).astype(BF16)


def panel32(work, p):
    r0 = 32 * p
    diag_tile = p // 4
    lane0 = r0 % 128
    tiles = [0, 1, 2] if p < 4 else [1, 2, 3]
    rows = {ti: [work[r0 + 8 * sg:r0 + 8 * sg + 8, 128 * ti:128 * ti + 128] for sg in range(4)] for ti in tiles}
    sub_id = lax.broadcasted_iota(jnp.int32, (8, 128), 0)

    def over_lanes(u, sg):
        return jnp.broadcast_to(rows[diag_tile][sg][:, lane0 + u:lane0 + u + 1], (8, 128))

    def over_sublanes(v, i):
        return jnp.broadcast_to(v[i:i + 1, :], (8, 128))

    col, fac = {}, {}
    for u in range(16):
        for sg in range(u // 8, 4):
            col[u, sg] = over_lanes(u, sg)
    for g in range(4):
        for t in range(8 * g, 8 * g + 8):
            tt = t - 8 * g
            rs = lax.rsqrt(over_sublanes(col[t, g], tt))
            for sg in range(g, 4):
                fac[t, sg] = col[t, sg] * rs
            for u in range(t + 1, min(8 * g + 16, 32)):
                ug = u // 8
                s = over_sublanes(fac[t, ug], u - 8 * ug)
                for sg in range(ug, 4):
                    col[u, sg] = col[u, sg] - fac[t, sg] * s
            for ti in tiles:
                row = over_sublanes(rows[ti][g], tt) * rs
                own = rows[ti][g] - fac[t, g] * row
                rows[ti][g] = jnp.where(sub_id > tt, own, jnp.where(sub_id == tt, row, rows[ti][g]))
                for sg in range(g + 1, 4):
                    rows[ti][sg] = rows[ti][sg] - fac[t, sg] * row
        if g < 2:
            for u in range(8 * g + 16, 8 * g + 24):
                for sg in range(u // 8, 4):
                    col[u, sg] = over_lanes(u, sg)
    for ti in tiles:
        for sg in range(4):
            work[r0 + 8 * sg:r0 + 8 * sg + 8, 128 * ti:128 * ti + 128] = rows[ti][sg]
    if p == 7:
        return
    high, mid, low = split3(jnp.concatenate([jnp.concatenate(rows[ti], axis=0) for ti in tiles], axis=1))
    first = (r0 + 32 - 128 * diag_tile) // 128 * 128
    rhs = jnp.concatenate([high, mid, high, mid, low, high], axis=0)
    lhs = jnp.concatenate([high, high, mid, mid, high, low], axis=0)[:, first:256 - 128 * diag_tile]
    upd = lax.dot_general(lhs, rhs, (((0,), (0,)), ((), ())), preferred_element_type=F32)
    skip = r0 + 32 - first - 128 * diag_tile
    for j, ti in enumerate(tiles):
        lanes = slice(128 * ti, 128 * ti + 128)
        work[r0 + 32:256, lanes] = work[r0 + 32:256, lanes] - upd[skip:, 128 * j:128 * j + 128]


def factor_kernel(*refs):
    blocks, (x_ref, own_l_ref, own_diag_ref, u_ref, work) = refs[:-5], refs[-5:]
    my_col, my_row = lax.axis_index("pc"), lax.axis_index("pr")
    row = lax.broadcasted_iota(jnp.int32, (NB, NB), 0)
    col = lax.broadcasted_iota(jnp.int32, (NB, NB), 1)
    for c in range(4):
        for r in range(4):
            if len(blocks) == 1:
                u_ref[NB * r:NB * r + NB, NB * c:NB * c + NB] = blocks[0][4 * c + r]
            else:
                at_row, at_col = (pl.ds(pl.multiple_of(v * NB, NB), NB) for v in (my_row ^ r, my_col ^ c))
                u_ref[at_row, at_col] = blocks[4 * c + r][...]
    x_ref[...] = jnp.zeros_like(x_ref)
    for b in range(4):
        a, e = NB * b, NB * b + NB
        work[:, :NB] = u_ref[a:e, a:e]
        work[:, NB:] = jnp.where(row == col, 1.0, 0.0)
        for p in range(8):
            panel32(work, p)
        ubb = jnp.where(col >= row, work[:, :NB], 0.0)
        xbb = jnp.where(col <= row, work[:, NB:], 0.0)
        u_ref[a:e, a:e] = ubb
        if b > 0:
            x_ref[a:e, :a] = dot(xbb, x_ref[a:e, :a])
            u_ref[a:e, :a] = jnp.zeros((NB, a), F32)
        x_ref[a:e, a:e] = xbb
        if b < 3:
            urow = dot(xbb, u_ref[a:e, e:])
            u_ref[a:e, e:] = urow
            for c in range(b + 1, 4):
                lo = NB * c
                uc = urow[:, lo - e:lo - e + NB]
                u_ref[lo:lo + NB, lo:] = u_ref[lo:lo + NB, lo:] - dot_tn(uc, urow[:, lo - e:])
                x_ref[lo:lo + NB, :e] = x_ref[lo:lo + NB, :e] - dot_tn(uc, x_ref[a:e, :e])
    at_row = pl.ds(pl.multiple_of(my_row * NB, NB), NB)
    at_col = pl.ds(pl.multiple_of(my_col * NB, NB), NB)
    own_l_ref[...] = u_ref[at_col, at_row].T
    own_diag_ref[...] = u_ref[at_row, at_row]


def call(kernel, flops, moved, **kw):
    cost = pl.CostEstimate(flops=flops, bytes_accessed=moved, transcendentals=0)
    return pl.pallas_call(kernel, cost_estimate=cost, compiler_params=pltpu.CompilerParams(vmem_limit_bytes=VMEM_LIMIT), **kw)


def shape(*dims):
    return jax.ShapeDtypeStruct(dims, F32)


def factor(blocks):
    vmem = pl.BlockSpec(memory_space=pltpu.VMEM)
    return call(
        factor_kernel, 30_000_000_000, 1 << 24,
        out_shape=(shape(SUP, SUP), shape(NB, NB), shape(NB, NB)), in_specs=[vmem] * len(blocks), out_specs=(vmem,) * 3,
        scratch_shapes=[pltpu.VMEM((SUP, SUP), F32), pltpu.VMEM((NB, 2 * NB), F32)],
    )(*blocks)


def flat_panel(panel):
    return panel.reshape(-1, 4, 2, 128).transpose(0, 2, 1, 3).reshape(-1, 128)


def unpack_kernel(in_ref, rest_ref):
    for n, s in enumerate((3, 2, 1)):
        for half in range(2):
            rest_ref[:, NB * n + 128 * half:NB * n + 128 * half + 128] = in_ref[pl.ds(4 * half + s, NB, stride=8), :]


def unpack(panel):
    rows = panel.shape[0] - NB
    return call(
        unpack_kernel, 1_000_000, 8 * rows * SUP, grid=(rows // NB,), out_shape=shape(rows, 3 * NB),
        in_specs=[pl.BlockSpec((8 * NB, 128), lambda i: (i + 1, 0))], out_specs=pl.BlockSpec((NB, 3 * NB), lambda i: (i, 0)),
    )(flat_panel(panel))


def pack_rows(i, cols, diags, out_ref):
    for s in range(4):
        def put(value, s=s):
            for half in range(2):
                out_ref[pl.ds(4 * half + s, NB, stride=8), :] = value[:, 128 * half:128 * half + 128]

        pl.when(i < s)(lambda: put(jnp.zeros((NB, NB), F32)))
        pl.when(i == s)(lambda s=s: put(diags[s][...]))
        pl.when(i > s)(lambda s=s: put(cols[s][...]))


def rows_kernel(split, own, y, z, top, bottom, x_ref, out_ref, own_ref, wide):
    my_col = lax.axis_index("pc")
    i = pl.program_id(0)

    def place(flip, ref):
        wide[:, pl.ds(pl.multiple_of((my_col ^ flip) * NB, NB), NB)] = ref[...]

    place(0, own)
    place(1, y)
    place(2, z)
    pl.when(i < split)(lambda: place(3, top))
    pl.when(i >= split)(lambda: place(3, bottom))
    for k in range(4):
        lanes = slice(NB * k, NB * k + NB)
        part = dot_nt(wide[:, lanes], x_ref[NB * k:, lanes])
        out_ref[:, NB * k:] = part if k == 0 else out_ref[:, NB * k:] + part
    own_ref[...] = out_ref[:, pl.ds(pl.multiple_of(my_col * NB, NB), NB)]


def solve_rows(pieces, x):
    own, _, _, _, _ = pieces
    rows = own.shape[0]
    tile = rows // 4
    split = 2
    block = pl.BlockSpec((tile, NB), lambda i: (i, 0))
    return call(
        functools.partial(rows_kernel, split), 30 * rows * SUP * SUP // 4, 12 * rows * SUP, grid=(4,),
        out_shape=(shape(rows, SUP), shape(rows, NB)),
        in_specs=[block, block, block, pl.BlockSpec((tile, NB), lambda i: (jnp.minimum(i, split - 1), 0)),
                  pl.BlockSpec((tile, NB), lambda i: (jnp.maximum(i - split, 0), 0)), pl.BlockSpec((SUP, SUP), lambda i: (0, 0))],
        out_specs=(pl.BlockSpec((tile, SUP), lambda i: (i, 0)), block),
        scratch_shapes=[pltpu.VMEM((tile, SUP), F32)],
    )(*pieces, x)


def cols_kernel(*refs):
    pieces, x_ref, outs, tall = refs[:4], refs[4], refs[5:-1], refs[-1]
    my_row = lax.axis_index("pr")
    i = pl.program_id(0)
    for j in range(4):
        tall[pl.ds(pl.multiple_of((my_row ^ j) * NB, NB), NB), :] = pieces[j][...]

    def put(ref):
        for k in range(4):
            e = NB * (k + 1)
            ref[NB * k:e, :] = dot(x_ref[NB * k:e, :e], tall[:e, :])

    if len(outs) == 1:
        put(outs[0])
    else:
        pl.when(i < 4)(lambda: put(outs[0]))
        pl.when(i >= 4)(lambda: put(outs[1]))


def solve_cols(pieces, x):
    cols = pieces[0].shape[1]
    outs = [shape(SUP, min(SUP, cols))] + ([shape(SUP, cols - SUP)] if cols > SUP else [])
    specs = [pl.BlockSpec((SUP, NB), lambda i: (0, jnp.minimum(i, min(SUP, cols) // NB - 1))), pl.BlockSpec((SUP, NB), lambda i: (0, jnp.maximum(i - 4, 0)))]
    return call(
        cols_kernel, 30 * cols * SUP * SUP // 4, 12 * cols * SUP, grid=(cols // NB,), out_shape=outs,
        in_specs=[pl.BlockSpec((NB, NB), lambda i: (0, i))] * 4 + [pl.BlockSpec((SUP, SUP), lambda i: (0, 0))],
        out_specs=specs[:len(outs)], scratch_shapes=[pltpu.VMEM((SUP, NB), F32)],
    )(*pieces, x)


def panel_kernel(*refs):
    rest_ref, l_ref, u_ref, diag_ref, col_ref = refs[:5]
    keep = rest_ref.shape[1] - NB
    new = rest_ref[...] - dot(l_ref[...], u_ref[...])
    i = pl.program_id(0)

    @pl.when(i == 0)
    def _():
        diag_ref[...] = new[:, keep:]
        if keep:
            refs[5][...] = new[:, :keep]

    @pl.when(i > 0)
    def _():
        col_ref[...] = new[:, keep:]
        if keep:
            refs[6][...] = new[:, :keep]


def update_panel(rest, l_rows, u_panel):
    rows, width = rest.shape
    keep = width - NB
    below = lambda i: (jnp.maximum(i - 1, 0), 0)
    zero = lambda i: (0, 0)
    outs = [shape(NB, NB), shape(rows - NB, NB)] + ([shape(NB, keep), shape(rows - NB, keep)] if keep else [])
    specs = [pl.BlockSpec((NB, NB), zero), pl.BlockSpec((NB, NB), below)]
    if keep:
        specs += [pl.BlockSpec((NB, keep), zero), pl.BlockSpec((NB, keep), below)]
    return call(
        panel_kernel, 12 * rows * width * SUP, 8 * rows * width + 4 * rows * SUP, grid=(rows // NB,), out_shape=outs,
        in_specs=[pl.BlockSpec((NB, width), lambda i: (i, 0)), pl.BlockSpec((NB, SUP), lambda i: (i, 0)), pl.BlockSpec((SUP, width), zero)],
        out_specs=specs,
    )(rest, l_rows, u_panel)


def row_kernel(*refs):
    trail_ref, l_ref, mine_ref, theirs_ref = refs[1:5]
    keep_ref, send_ref = refs[-2:]
    j = pl.program_id(0)

    @pl.when(j == 0)
    def _():
        keep_ref[:, :SUP] = trail_ref[...] - dot(l_ref[...], mine_ref[...])
        if len(refs) == 8:
            keep_ref[:, SUP:] = refs[5][...]
            send_ref[:, SUP:] = refs[5][...]

    @pl.when(j == 1)
    def _():
        send_ref[:, :SUP] = trail_ref[...] - dot(l_ref[...], theirs_ref[...])


def update_row(core, trail, l_rows, mine, theirs, panel_row, step):
    extra = [] if panel_row is None else [panel_row]
    width = SUP + (0 if panel_row is None else panel_row.shape[1])
    whole = lambda a: pl.BlockSpec(a.shape, lambda j, h: (0, 0))
    out = pl.BlockSpec((NB, width), lambda j, h: (0, 0))
    return call(
        row_kernel, 24 * NB * SUP * SUP, 12 * SUP * SUP,
        grid_spec=pltpu.PrefetchScalarGridSpec(
            num_scalar_prefetch=1, grid=(2,),
            in_specs=[pl.BlockSpec((NB, SUP), lambda j, h: (step + 1, h[0] ^ j)), pl.BlockSpec((NB, SUP), lambda j, h: (0, 0)),
                      whole(mine), whole(theirs)] + [whole(a) for a in extra],
            out_specs=(out, out)),
        out_shape=(shape(NB, width), shape(NB, width)),
    )(core, trail, l_rows, mine, theirs, *extra)


def trail_kernel(core_ref, trail_ref, l_ref, mine_ref, theirs_ref, diag_ref, *rest):
    my_row = lax.axis_index("pr")
    j, i = pl.program_id(0), pl.program_id(1)
    out_ref = rest[0]
    if len(rest) > 1:
        out_ref = rest[8]
        pack_rows(jnp.minimum(j * pl.num_programs(1) + i, pl.num_programs(1) + 2), rest[:4], rest[4:8], rest[9])

    def go(u_ref):
        @pl.when(i == 0)
        def _():
            own = u_ref[pl.ds(pl.multiple_of(my_row * NB, NB), NB), :]
            out_ref[...] = dot_tn(diag_ref[...], own)

        @pl.when(i > 0)
        def _():
            out_ref[...] = trail_ref[...] - dot(l_ref[...], u_ref[...])

    pl.when(j == 0)(lambda: go(mine_ref))
    pl.when(j == 1)(lambda: go(theirs_ref))


def update_trail(core, trail, l_rows, mine, theirs, own_diag, step, out_cols=(), out_diags=()):
    rows, cols = trail.shape
    off = 1 if step < 3 else 0
    count = rows // NB - step - off
    at = pl.BlockSpec((NB, SUP), lambda j, i, h: (jnp.where(i == 0, step, step + off + i), h[0] ^ j))
    whole = pl.BlockSpec((SUP, SUP), lambda j, i, h: (0, 0))
    ins = [at, pl.BlockSpec((NB, SUP), lambda j, i, h: (jnp.maximum(i, 1) - 1 + off, 0)), whole, whole,
           pl.BlockSpec((NB, NB), lambda j, i, h: (0, 0))]
    outs, shapes = [at], [shape(rows, cols)]
    if out_cols:
        block = lambda j, i: jnp.minimum(j * count + i, rows // NB - 1)
        ins += [pl.BlockSpec((NB, NB), lambda j, i, h, s=s: (jnp.maximum(block(j, i) - s - 1, 0), 0)) for s in range(4)]
        ins += [pl.BlockSpec((NB, NB), lambda j, i, h: (0, 0))] * 4
        outs.append(pl.BlockSpec((8 * NB, 128), lambda j, i, h: (block(j, i), 0)))
        shapes.append(shape(rows * 8, 128))
    return call(
        trail_kernel, 12 * count * NB * cols * SUP, 8 * count * NB * cols,
        grid_spec=pltpu.PrefetchScalarGridSpec(num_scalar_prefetch=1, grid=(2, count), in_specs=ins, out_specs=outs),
        out_shape=shapes, input_output_aliases={1: 0} if step else {},
    )(core, trail, l_rows, mine, theirs, own_diag, *out_cols, *out_diags)


FLIP1 = [(0, 1), (1, 0), (2, 3), (3, 2)]
FLIP2 = [(0, 2), (2, 0), (1, 3), (3, 1)]
FLIP3 = [(0, 3), (3, 0), (1, 2), (2, 1)]


def gather_diag(block):
    got = {(0, 0): block}
    for jc in range(4):
        for jr in (0, 2):
            if (jc, jr) != (0, 0):
                perm = [(4 * c + r, 4 * (c ^ jc) + (r ^ jr)) for c in range(4) for r in range(4)]
                got[jc, jr] = lax.ppermute(block, ("pc", "pr"), perm)
    for jc in range(4):
        for jr in (0, 2):
            got[jc, jr + 1] = lax.ppermute(got[jc, jr], "pr", FLIP1)
    return [got[jc, jr] for jc in range(4) for jr in range(4)]


def gather_cols(keep, send):
    return [keep, lax.ppermute(send, "pr", FLIP1), lax.ppermute(keep, "pr", FLIP2), lax.ppermute(send, "pr", FLIP3)]


def gather_all(panel):
    x = lax.ppermute(panel, "pr", FLIP2)
    return [panel, lax.ppermute(panel, "pr", FLIP1), x, lax.ppermute(x, "pr", FLIP1)]


def solution(mesh):
    def local_part(panel_tile, trail_tile):
        my_row = lax.axis_index("pr")
        half = my_row % 2
        core = jnp.full((1,), half, jnp.int32)
        trail = trail_tile
        out_cols, out_diags = [], []
        for step in range(4):
            if step == 0:
                blocks = gather_diag(panel_tile[:NB, 0, :])
                col_panel = panel_tile[NB:, 0, :]
                keep, send = (lax.dynamic_slice(trail_tile, (0, SUP * h), (NB, SUP)) for h in (half, 1 - half))
                panel_row = jnp.concatenate([panel_tile[:NB, s, :] for s in (3, 2, 1)], axis=1)
                rest = unpack(panel_tile)
            else:
                blocks = [lax.all_gather(diag_block, ("pc", "pr"))]
            y = lax.ppermute(col_panel, "pc", FLIP1)
            z = lax.ppermute(col_panel, "pc", FLIP2)
            col_pieces = gather_cols(keep, send)
            if step == 0:
                row_pieces = gather_all(panel_row)
            if step:
                trail, = update_trail(core, trail, l_rows, mine, theirs, own_diag, step - 1)
                blocks, y, z, trail = lax.optimization_barrier((blocks, y, z, trail))
            split = col_panel.shape[0] // 2
            top = lax.ppermute(z[:split], "pc", FLIP1)
            bottom = lax.ppermute(y[split:], "pc", FLIP2)
            x_sup, own_l, own_diag = factor(blocks)
            mine, *more = solve_cols(col_pieces, x_sup)
            if step == 0:
                more = solve_cols(row_pieces, x_sup)
            theirs = lax.ppermute(mine, "pr", FLIP1)
            l_rows, own_col = solve_rows([col_panel, y, z, top, bottom], x_sup)
            out_cols.append(own_col)
            out_diags.append(own_l)
            if step < 3:
                diag_block, col_panel, *left = update_panel(rest, l_rows, more[0])
                panel_row, rest = left if left else (None, None)
                keep, send = update_row(core, trail, l_rows, mine, theirs, panel_row, step)
        trail, flat = update_trail(core, trail, l_rows, mine, theirs, own_diag, 3, out_cols, out_diags)
        rows = trail.shape[0]
        return flat.reshape(rows, 2, 4, 128).transpose(0, 2, 1, 3).reshape(rows, 4, NB), trail

    spec_panel = P("pr", "pc", None)
    spec_trail = P("pr", "pc")
    return jax.shard_map(local_part, mesh=mesh, in_specs=(spec_panel, spec_trail), out_specs=(spec_panel, spec_trail), check_vma=False)
```

```python
import functools

import jax
import jax.numpy as jnp
from jax import lax
from jax.experimental import pallas as pl
from jax.experimental.pallas import tpu as pltpu
from jax.sharding import PartitionSpec as P


F32 = jnp.float32
BF16 = jnp.bfloat16
HIGH = lax.Precision.HIGHEST
NB = 256
SUP = 1024
MIB = 1024 * 1024


def dot(a, b):
    return lax.dot_general(a, b, (((1,), (0,)), ((), ())), precision=HIGH, preferred_element_type=F32)


def dot_nt(a, b):
    return lax.dot_general(a, b, (((1,), (1,)), ((), ())), precision=HIGH, preferred_element_type=F32)


def dot_tn(a, b):
    return lax.dot_general(a, b, (((0,), (0,)), ((), ())), precision=HIGH, preferred_element_type=F32)


def split3(x):
    high = x.astype(BF16)
    rest = x - high.astype(F32)
    mid = rest.astype(BF16)
    return high, mid, (rest - mid.astype(F32)).astype(BF16)


def panel32(work, p, filler=lambda k: None):
    r0 = 32 * p
    diag_tile = p // 4
    lane0 = r0 % 128
    tiles = [0, 1, 2] if p < 4 else [1, 2, 3]
    rows = {ti: [work[r0 + 8 * sg:r0 + 8 * sg + 8, 128 * ti:128 * ti + 128] for sg in range(4)] for ti in tiles}
    sub_id = lax.broadcasted_iota(jnp.int32, (8, 128), 0)

    def over_lanes(u, sg):
        return jnp.broadcast_to(rows[diag_tile][sg][:, lane0 + u:lane0 + u + 1], (8, 128))

    def over_sublanes(v, i):
        return jnp.broadcast_to(v[i:i + 1, :], (8, 128))

    col, fac = {}, {}
    for u in range(16):
        for sg in range(u // 8, 4):
            col[u, sg] = over_lanes(u, sg)
    for g in range(4):
        if g < 3:
            filler(g)
        for t in range(8 * g, 8 * g + 8):
            tt = t - 8 * g
            rs = lax.rsqrt(over_sublanes(col[t, g], tt))
            for sg in range(g, 4):
                fac[t, sg] = col[t, sg] * rs
            for u in range(t + 1, min(8 * g + 16, 32)):
                ug = u // 8
                s = over_sublanes(fac[t, ug], u - 8 * ug)
                for sg in range(ug, 4):
                    col[u, sg] = col[u, sg] - fac[t, sg] * s
            for ti in tiles:
                row = over_sublanes(rows[ti][g], tt) * rs
                own = rows[ti][g] - fac[t, g] * row
                rows[ti][g] = jnp.where(sub_id > tt, own, jnp.where(sub_id == tt, row, rows[ti][g]))
                for sg in range(g + 1, 4):
                    rows[ti][sg] = rows[ti][sg] - fac[t, sg] * row
        if g < 2:
            for u in range(8 * g + 16, 8 * g + 24):
                for sg in range(u // 8, 4):
                    col[u, sg] = over_lanes(u, sg)
    for ti in tiles:
        for sg in range(4):
            work[r0 + 8 * sg:r0 + 8 * sg + 8, 128 * ti:128 * ti + 128] = rows[ti][sg]
    if p == 7:
        filler(3)
        return
    high, mid, low = split3(jnp.concatenate([jnp.concatenate(rows[ti], axis=0) for ti in tiles], axis=1))
    first = (r0 + 32 - 128 * diag_tile) // 128 * 128
    rhs = jnp.concatenate([high, mid, high, mid, low, high], axis=0)
    lhs = jnp.concatenate([high, high, mid, mid, high, low], axis=0)[:, first:256 - 128 * diag_tile]
    upd = lax.dot_general(lhs, rhs, (((0,), (0,)), ((), ())), preferred_element_type=F32)
    filler(3)
    skip = r0 + 32 - first - 128 * diag_tile
    for j, ti in enumerate(tiles):
        lanes = slice(128 * ti, 128 * ti + 128)
        work[r0 + 32:256, lanes] = work[r0 + 32:256, lanes] - upd[skip:, 128 * j:128 * j + 128]


def spread_factor(b, u_ref, x_ref, work):
    row = lax.broadcasted_iota(jnp.int32, (NB, NB), 0)
    col = lax.broadcasted_iota(jnp.int32, (NB, NB), 1)
    a, e = NB * b, NB * b + NB
    xbb = jnp.where(col <= row, work[:, NB:], 0.0)
    u_ref[a:e, a:e] = jnp.where(col >= row, work[:, :NB], 0.0)
    if b > 0:
        x_ref[a:e, :a] = dot(xbb, x_ref[a:e, :a])
        u_ref[a:e, :a] = jnp.zeros((NB, a), F32)
    x_ref[a:e, a:e] = xbb
    if b < 3:
        urow = dot(xbb, u_ref[a:e, e:])
        u_ref[a:e, e:] = urow
        for c in range(b + 1, 4):
            lo = NB * c
            uc = urow[:, lo - e:lo - e + NB]
            u_ref[lo:lo + NB, lo:] = u_ref[lo:lo + NB, lo:] - dot_tn(uc, urow[:, lo - e:])
            x_ref[lo:lo + NB, :e] = x_ref[lo:lo + NB, :e] - dot_tn(uc, x_ref[a:e, :e])


def factor_block(b, u_ref, x_ref, own_l_ref, own_diag_ref, work, filler=lambda p, k: None):
    row = lax.broadcasted_iota(jnp.int32, (NB, NB), 0)
    col = lax.broadcasted_iota(jnp.int32, (NB, NB), 1)
    at = pl.ds(pl.multiple_of(b * NB, NB), NB)
    work[:, :NB] = u_ref[at, at]
    work[:, NB:] = jnp.where(row == col, 1.0, 0.0)
    for p in range(8):
        panel32(work, p, functools.partial(filler, p))
    for n in range(4):
        pl.when(b == n)(lambda n=n: spread_factor(n, u_ref, x_ref, work))

    @pl.when(b == 3)
    def _():
        at_row, at_col = (pl.ds(pl.multiple_of(lax.axis_index(name) * NB, NB), NB) for name in ("pr", "pc"))
        own_l_ref[...] = u_ref[at_col, at_row].T
        own_diag_ref[...] = u_ref[at_row, at_row]


def factor_kernel(*refs):
    blocks, (x_ref, own_l_ref, own_diag_ref, u_ref, work) = refs[:-5], refs[-5:]
    my_col, my_row = lax.axis_index("pc"), lax.axis_index("pr")
    b = pl.program_id(0)

    @pl.when(b == 0)
    def _():
        for c in range(4):
            for r in range(4):
                at_row, at_col = (pl.ds(pl.multiple_of(v * NB, NB), NB) for v in (my_row ^ r, my_col ^ c))
                u_ref[at_row, at_col] = blocks[r % 2][c + 4 * (r // 2)]
        x_ref[...] = jnp.zeros_like(x_ref)

    factor_block(b, u_ref, x_ref, own_l_ref, own_diag_ref, work)


def call(kernel, flops, moved, vmem, **kw):
    cost = pl.CostEstimate(flops=flops, bytes_accessed=moved, transcendentals=0)
    return pl.pallas_call(kernel, cost_estimate=cost, compiler_params=pltpu.CompilerParams(vmem_limit_bytes=vmem * MIB), **kw)


def in_hbm(x):
    return pltpu.with_memory_space_constraint(x, pltpu.HBM)


def shape(*dims):
    return pltpu.HBM(dims, F32)


def near(*dims):
    return jax.ShapeDtypeStruct(dims, F32)


def factor(blocks):
    vmem = pl.BlockSpec(memory_space=pltpu.VMEM)
    return call(
        factor_kernel, 30_000_000_000, 1 << 24, 20, grid=(4,),
        out_shape=(near(SUP, SUP), shape(NB, NB), shape(NB, NB)), in_specs=[vmem] * len(blocks), out_specs=(vmem,) * 3,
        scratch_shapes=[pltpu.VMEM((SUP, SUP), F32), pltpu.VMEM((NB, 2 * NB), F32)],
    )(*blocks)


def flat_panel(panel):
    return panel.reshape(-1, 4, 2, 128).transpose(0, 2, 1, 3).reshape(-1, 128)


def dot_parts(a, b):
    total = None
    for i, j in ((2, 0), (0, 2), (1, 1), (1, 0), (0, 1), (0, 0)):
        product = lax.dot_general(a(i), b(j), (((1,), (0,)), ((), ())), preferred_element_type=F32)
        total = product if total is None else total + product
    return total


def fused_kernel(s_ref, trail_ref, l_ref, mine_ref, theirs_ref, *rest):
    x_ref, own_l_ref, own_diag_ref, out_ref, u_ref, work, u_parts, l_parts, landing, block_sem, land_sem = rest[-11:]
    b = pl.program_id(0)
    my_row = lax.axis_index("pr")

    def landing_copy(k, w):
        at = pl.ds(128 * k, 128)
        return pltpu.make_async_copy((mine_ref, theirs_ref)[w].at[at], landing.at[w, at], land_sem.at[2 * k + w])

    def block_copy(n):
        return pltpu.make_async_copy(s_ref.at[n], u_ref.at[pl.ds(n % 4 * NB, NB), pl.ds(n // 4 * NB, NB)], block_sem.at[n])

    @pl.when(b == 0)
    def _():
        half = my_row % 2
        for k in range(8):
            for w in range(2):
                landing_copy(k, w).start()
        for n in range(16):
            block_copy(n).start()
        x_ref[...] = jnp.zeros_like(x_ref)
        for k in range(8):
            for w in range(2):
                landing_copy(k, w).wait()

                def split_rows(i, carry, k=k, w=w):
                    at = pl.ds(pl.multiple_of(128 * k + 32 * i, 32), 32)
                    for n, part in enumerate(split3(landing[w, at, :])):
                        u_parts[n, at, pl.ds(pl.multiple_of((half ^ w) * SUP, SUP), SUP)] = part
                    return carry

                lax.fori_loop(0, 4, split_rows, 0)
        for n in range(16):
            block_copy(n).wait()

    for n, part in enumerate(split3(l_ref[...])):
        l_parts[n] = part

    def piece(q, k):
        deep, lanes = slice(NB * k, NB * k + NB), slice(NB * q, NB * q + NB)
        total = dot_parts(lambda i: l_parts[i, :, deep], lambda j: u_parts[j, deep, lanes])
        out_ref[:, lanes] = (trail_ref if k == 0 else out_ref)[:, lanes] - total

    factor_block(b, u_ref, x_ref, own_l_ref, own_diag_ref, work, piece)


def factor_beside(blocks, source, trail, l_rows, mine, theirs):
    rows, cols = trail.shape
    last = rows // NB - 4
    ahead = l_rows.shape[0] // NB - 4
    vmem = pl.BlockSpec(memory_space=pltpu.VMEM)
    at = pl.BlockSpec((NB, cols), lambda b: (last + b, 0))
    anywhere = pl.BlockSpec(memory_space=pl.ANY)
    operands = [in_hbm(blocks), trail if source is None else source, in_hbm(l_rows), in_hbm(mine), in_hbm(theirs)]
    specs = [anywhere, at, pl.BlockSpec((NB, SUP), lambda b: (ahead + b, 0)), anywhere, anywhere]
    if source is not None:
        operands.append(trail)
        specs.append(anywhere)
    scratch = [pltpu.VMEM((SUP, SUP), F32), pltpu.VMEM((NB, 2 * NB), F32), pltpu.VMEM((3, SUP, cols), BF16), pltpu.VMEM((3, NB, SUP), BF16),
               pltpu.VMEM((2, SUP, SUP), F32), pltpu.SemaphoreType.DMA((16,)), pltpu.SemaphoreType.DMA((16,))]
    return call(
        fused_kernel, 100_000_000_000, 1 << 25, 48, grid=(4,),
        out_shape=(near(SUP, SUP), shape(NB, NB), shape(NB, NB), shape(rows, cols)), in_specs=specs, out_specs=(vmem, vmem, vmem, at),
        scratch_shapes=scratch,
        input_output_aliases={1 if source is None else 5: 3},
    )(*operands)


def unpack_kernel(in_ref, rest_ref):
    for n, s in enumerate((3, 2, 1)):
        for half in range(2):
            rest_ref[:, NB * n + 128 * half:NB * n + 128 * half + 128] = in_ref[pl.ds(4 * half + s, NB, stride=8), :]


def unpack(panel):
    rows = panel.shape[0] - NB
    return call(
        unpack_kernel, 1_000_000, 8 * rows * SUP, 12, grid=(rows // NB,), out_shape=shape(rows, 3 * NB),
        in_specs=[pl.BlockSpec((8 * NB, 128), lambda i: (i + 1, 0))], out_specs=pl.BlockSpec((NB, 3 * NB), lambda i: (i, 0)),
    )(flat_panel(panel))


def pack_rows(i, cols, diags, out_ref):
    for s in range(4):
        def put(value, s=s):
            for half in range(2):
                out_ref[pl.ds(4 * half + s, NB, stride=8), :] = value[:, 128 * half:128 * half + 128]

        pl.when(i < s)(lambda: put(jnp.zeros((NB, NB), F32)))
        pl.when(i == s)(lambda s=s: put(diags[s][...]))
        pl.when(i > s)(lambda s=s: put(cols[s][...]))


def rows_kernel(split, own, y, z, top, bottom, x_ref, out_ref, own_ref, wide):
    my_col = lax.axis_index("pc")
    i = pl.program_id(0)

    def place(flip, ref):
        wide[:, pl.ds(pl.multiple_of((my_col ^ flip) * NB, NB), NB)] = ref[...]

    place(0, own)
    place(1, y)
    place(2, z)
    pl.when(i < split)(lambda: place(3, top))
    pl.when(i >= split)(lambda: place(3, bottom))
    for k in range(4):
        lanes = slice(NB * k, NB * k + NB)
        part = dot_nt(wide[:, lanes], x_ref[NB * k:, lanes])
        out_ref[:, NB * k:] = part if k == 0 else out_ref[:, NB * k:] + part
    own_ref[...] = out_ref[:, pl.ds(pl.multiple_of(my_col * NB, NB), NB)]


def solve_rows(pieces, x):
    own, y, z, top, bottom = pieces
    rows = own.shape[0]
    tile = rows // 4
    split = 2
    block = pl.BlockSpec((tile, NB), lambda i: (i, 0))
    return call(
        functools.partial(rows_kernel, split), 30 * rows * SUP * SUP // 4, 12 * rows * SUP, 34, grid=(4,),
        out_shape=(shape(rows, SUP), shape(rows, NB)),
        in_specs=[block, block, block, pl.BlockSpec((tile, NB), lambda i: (jnp.minimum(i, split - 1), 0)),
                  pl.BlockSpec((tile, NB), lambda i: (jnp.maximum(i - split, 0), 0)), pl.BlockSpec((SUP, SUP), lambda i: (0, 0))],
        out_specs=(pl.BlockSpec((tile, SUP), lambda i: (i, 0)), block),
        scratch_shapes=[pltpu.VMEM((tile, SUP), F32)],
    )(in_hbm(own), y, z, top, bottom, x)


def cols_kernel(*refs):
    pieces, x_ref, outs, tall = refs[:4], refs[4], refs[5:-1], refs[-1]
    my_row = lax.axis_index("pr")
    i = pl.program_id(0)
    for j in range(4):
        tall[pl.ds(pl.multiple_of((my_row ^ j) * NB, NB), NB), :] = pieces[j][...]

    parts = [dot(x_ref[NB * k:NB * k + NB, :NB * k + NB], tall[:NB * k + NB, :]) for k in range(4)]

    def put(ref):
        for k in range(4):
            ref[NB * k:NB * k + NB, :] = parts[k]

    if len(outs) == 1:
        put(outs[0])
    else:
        pl.when(i < 4)(lambda: put(outs[0]))
        pl.when(i >= 4)(lambda: put(outs[1]))


def solve_cols(pieces, x):
    cols = pieces[0].shape[1]
    outs = [shape(SUP, min(SUP, cols))] + ([near(SUP, cols - SUP)] if cols > SUP else [])
    specs = [pl.BlockSpec((SUP, NB), lambda i: (0, jnp.minimum(i, min(SUP, cols) // NB - 1))), pl.BlockSpec((SUP, NB), lambda i: (0, jnp.maximum(i - 4, 0)))]
    return call(
        cols_kernel, 30 * cols * SUP * SUP // 4, 12 * cols * SUP, 20, grid=(cols // NB,), out_shape=outs,
        in_specs=[pl.BlockSpec((NB, NB), lambda i: (0, i))] * 4 + [pl.BlockSpec((SUP, SUP), lambda i: (0, 0))],
        out_specs=specs[:len(outs)], scratch_shapes=[pltpu.VMEM((SUP, NB), F32)],
    )(*pieces, x)


def panel_kernel(*refs):
    rest_ref, l_ref, u_ref, diag_ref, col_ref = refs[:5]
    keep = rest_ref.shape[1] - NB
    new = rest_ref[...] - dot(l_ref[...], u_ref[...])
    i = pl.program_id(0)

    @pl.when(i == 0)
    def _():
        diag_ref[...] = new[:, keep:]
        if keep:
            refs[5][...] = new[:, :keep]

    @pl.when(i > 0)
    def _():
        col_ref[...] = new[:, keep:]
        if keep:
            refs[6][...] = new[:, :keep]


def update_panel(rest, l_rows, u_panel):
    rows, width = rest.shape
    keep = width - NB
    below = lambda i: (jnp.maximum(i - 1, 0), 0)
    zero = lambda i: (0, 0)
    outs = [shape(NB, NB), shape(rows - NB, NB)] + ([shape(NB, keep), shape(rows - NB, keep)] if keep else [])
    specs = [pl.BlockSpec((NB, NB), zero), pl.BlockSpec((NB, NB), below)]
    if keep:
        specs += [pl.BlockSpec((NB, keep), zero), pl.BlockSpec((NB, keep), below)]
    return call(
        panel_kernel, 12 * rows * width * SUP, 8 * rows * width + 4 * rows * SUP, 20, grid=(rows // NB,), out_shape=outs,
        in_specs=[pl.BlockSpec((NB, width), lambda i: (i, 0)), pl.BlockSpec((NB, SUP), lambda i: (i, 0)), pl.BlockSpec((SUP, width), zero)],
        out_specs=specs,
    )(in_hbm(rest), in_hbm(l_rows), u_panel)


def row_kernel(*refs):
    trail_ref, l_ref, mine_ref, theirs_ref = refs[1:5]
    keep_ref, send_ref, landing, sem = refs[-4:]
    j = pl.program_id(0)
    copies = [pltpu.make_async_copy(ref, landing.at[n], sem.at[n]) for n, ref in enumerate((mine_ref, theirs_ref))]

    @pl.when(j == 0)
    def _():
        for copy in copies:
            copy.start()
        if len(refs) == 10:
            keep_ref[:, SUP:] = refs[5][...]
            send_ref[:, SUP:] = refs[5][...]

    for n, copy in enumerate(copies):
        pl.when(j == n)(copy.wait)
    new = trail_ref[...] - dot(l_ref[...], landing[j])

    @pl.when(j == 0)
    def _():
        keep_ref[:, :SUP] = new

    @pl.when(j == 1)
    def _():
        send_ref[:, :SUP] = new


def update_row(core, trail, l_rows, mine, theirs, panel_row, step):
    extra = [] if panel_row is None else [panel_row]
    width = SUP + (0 if panel_row is None else panel_row.shape[1])
    out = pl.BlockSpec((NB, width), lambda j, h: (0, 0))
    anywhere = pl.BlockSpec(memory_space=pl.ANY)
    return call(
        row_kernel, 24 * NB * SUP * SUP, 12 * SUP * SUP, 30,
        grid_spec=pltpu.PrefetchScalarGridSpec(
            num_scalar_prefetch=1, grid=(2,),
            in_specs=[pl.BlockSpec((NB, SUP), lambda j, h: (step + 1, h[0] ^ j)), pl.BlockSpec((NB, SUP), lambda j, h: (0, 0)),
                      anywhere, anywhere] + [pl.BlockSpec(a.shape, lambda j, h: (0, 0)) for a in extra],
            out_specs=(out, out), scratch_shapes=[pltpu.VMEM((2, SUP, SUP), F32), pltpu.SemaphoreType.DMA((2,))]),
        out_shape=(shape(NB, width), shape(NB, width)),
    )(core, trail, in_hbm(l_rows), in_hbm(mine), in_hbm(theirs), *extra)


def trail_kernel(core_ref, trail_ref, l_ref, mine_ref, theirs_ref, diag_ref, *rest):
    rest, (landing, u_parts, l_parts, sem) = rest[:-4], rest[-4:]
    my_row = lax.axis_index("pr")
    j, i = pl.program_id(0), pl.program_id(1)
    copies = [pltpu.make_async_copy(ref, landing, sem.at[n]) for n, ref in enumerate((mine_ref, theirs_ref))]
    out_ref = rest[0]
    if len(rest) > 1:
        out_ref = rest[8]
        pack_rows(jnp.minimum(j * pl.num_programs(1) + i, pl.num_programs(1) + 2), rest[:4], rest[4:8], rest[9])

    @pl.when(i == 0)
    def _():
        pl.when(j == 0)(copies[0].start)
        pl.when(j == 0)(copies[0].wait)
        pl.when(j == 1)(copies[1].wait)

        def split_rows(k, carry):
            at = pl.ds(pl.multiple_of(k * 64, 64), 64)
            for n, part in enumerate(split3(landing[at, :])):
                u_parts[n, at, :] = part
            return carry

        lax.fori_loop(0, SUP // 64, split_rows, 0)
        out_ref[...] = dot_tn(diag_ref[...], landing[pl.ds(pl.multiple_of(my_row * NB, NB), NB), :])

    @pl.when(i > 0)
    def _():
        pl.when((i == 1) & (j == 0))(copies[1].start)
        for n, part in enumerate(split3(l_ref[...])):
            l_parts[n] = part
        out_ref[...] = trail_ref[...] - dot_parts(lambda n: l_parts[n], lambda n: u_parts[n])


def update_trail(core, trail, l_rows, mine, theirs, own_diag, step, out_cols=(), out_diags=()):
    rows, cols = trail.shape
    off = 1 if step < 3 else 0
    count = rows // NB - step - off - (4 if step < 3 else 0)
    at = pl.BlockSpec((NB, SUP), lambda j, i, h: (jnp.where(i == 0, step, step + off + i), h[0] ^ j))
    anywhere = pl.BlockSpec(memory_space=pl.ANY)
    ins = [at, pl.BlockSpec((NB, SUP), lambda j, i, h: (jnp.maximum(i, 1) - 1 + off, 0)), anywhere, anywhere,
           pl.BlockSpec((NB, NB), lambda j, i, h: (0, 0))]
    outs, shapes = [at], [shape(rows, cols)]
    if out_cols:
        block = lambda j, i: jnp.minimum(j * count + i, rows // NB - 1)
        ins += [pl.BlockSpec((NB, NB), lambda j, i, h, s=s: (jnp.maximum(block(j, i) - s - 1, 0), 0)) for s in range(4)]
        ins += [pl.BlockSpec((NB, NB), lambda j, i, h: (0, 0))] * 4
        outs.append(pl.BlockSpec((8 * NB, 128), lambda j, i, h: (block(j, i), 0)))
        shapes.append(shape(rows * 8, 128))
    return call(
        trail_kernel, 12 * count * NB * cols * SUP, 8 * count * NB * cols, 32,
        grid_spec=pltpu.PrefetchScalarGridSpec(num_scalar_prefetch=1, grid=(2, count), in_specs=ins, out_specs=outs, scratch_shapes=[
            pltpu.VMEM((SUP, SUP), F32), pltpu.VMEM((3, SUP, SUP), BF16), pltpu.VMEM((3, NB, SUP), BF16), pltpu.SemaphoreType.DMA((2,))]),
        out_shape=shapes, input_output_aliases={1: 0} if step else {},
    )(core, trail, in_hbm(l_rows), in_hbm(mine), in_hbm(theirs), *(in_hbm(a) for a in (own_diag, *out_cols, *out_diags)))


FLIP1 = [(0, 1), (1, 0), (2, 3), (3, 2)]
FLIP2 = [(0, 2), (2, 0), (1, 3), (3, 1)]
FLIP3 = [(0, 3), (3, 0), (1, 2), (2, 1)]


def gather_diag(block):
    have = block[None]
    for axis, perm in (("pc", FLIP1), ("pc", FLIP2), ("pr", FLIP2)):
        have = jnp.concatenate([have, lax.ppermute(have, axis, perm)], axis=0)
    return [have, lax.ppermute(have, "pr", FLIP1)]


def gather_cols(keep, send):
    return [keep, lax.ppermute(send, "pr", FLIP1), lax.ppermute(keep, "pr", FLIP2), lax.ppermute(send, "pr", FLIP3)]


def gather_all(panel):
    x = lax.ppermute(panel, "pr", FLIP2)
    other = lax.ppermute(panel, "pr", FLIP1)
    return [panel, other, x, lax.ppermute(x, "pr", FLIP1)]


def solution(mesh):
    def local_part(panel_tile, trail_tile):
        my_row = lax.axis_index("pr")
        half = my_row % 2
        core = jnp.full((1,), half, jnp.int32)
        trail = trail_tile
        out_cols, out_diags = [], []
        for step in range(4):
            if step == 0:
                diag_block, later = lax.optimization_barrier((panel_tile[:NB, 0, :], panel_tile))
                blocks = gather_diag(diag_block)
                col_panel = later[NB:, 0, :]
                keep, send = (lax.dynamic_slice(trail_tile, (0, SUP * h), (NB, SUP)) for h in (half, 1 - half))
                panel_row = jnp.concatenate([later[:NB, s, :] for s in (3, 2, 1)], axis=1)
                rest = unpack(panel_tile)
            else:
                blocks = [lax.all_gather(diag_block, ("pc", "pr"))]
            y = lax.ppermute(col_panel, "pc", FLIP1)
            z = lax.ppermute(col_panel, "pc", FLIP2)
            col_pieces = gather_cols(keep, send)
            if step == 0:
                row_pieces = gather_all(panel_row)
            if step:
                source = trail if step == 1 else None
                trail, = update_trail(core, trail, l_rows, mine, theirs, own_diag, step - 1)
                blocks, y, z, trail = lax.optimization_barrier((blocks, y, z, trail))
            split = col_panel.shape[0] // 2
            top = lax.ppermute(z[:split], "pc", FLIP1)
            bottom = lax.ppermute(y[split:], "pc", FLIP2)
            if step == 0:
                x_sup, own_l, own_diag = factor(blocks)
            else:
                x_sup, own_l, own_diag, trail = factor_beside(*blocks, source, trail, l_rows, mine, theirs)
            mine, *more = solve_cols(col_pieces, x_sup)
            if step == 0:
                more = solve_cols(row_pieces, x_sup)
            theirs = lax.ppermute(mine, "pr", FLIP1)
            l_rows, own_col = solve_rows([col_panel, y, z, top, bottom], x_sup)
            out_cols.append(own_col)
            out_diags.append(own_l)
            if step < 3:
                diag_block, col_panel, *left = update_panel(rest, l_rows, more[0])
                panel_row, rest = left if left else (None, None)
                keep, send = update_row(core, trail, l_rows, mine, theirs, panel_row, step)
        trail, flat = update_trail(core, trail, l_rows, mine, theirs, own_diag, 3, out_cols, out_diags)
        rows = trail.shape[0]
        return flat.reshape(rows, 2, 4, 128).transpose(0, 2, 1, 3).reshape(rows, 4, NB), trail

    spec_panel = P("pr", "pc", None)
    spec_trail = P("pr", "pc")
    return jax.shard_map(local_part, mesh=mesh, in_specs=(spec_panel, spec_trail), out_specs=(spec_panel, spec_trail), check_vma=False)
```

```python
import functools

import jax
import jax.numpy as jnp
from jax import lax
from jax.experimental import pallas as pl
from jax.experimental.pallas import tpu as pltpu
from jax.sharding import PartitionSpec as P


F32 = jnp.float32
BF16 = jnp.bfloat16
HIGH = lax.Precision.HIGHEST
NB = 256
SUP = 1024
MIB = 1024 * 1024


def dot(a, b):
    return lax.dot_general(a, b, (((1,), (0,)), ((), ())), precision=HIGH, preferred_element_type=F32)


def dot_nt(a, b):
    return lax.dot_general(a, b, (((1,), (1,)), ((), ())), precision=HIGH, preferred_element_type=F32)


def dot_tn(a, b):
    return lax.dot_general(a, b, (((0,), (0,)), ((), ())), precision=HIGH, preferred_element_type=F32)


def split3(x):
    high = x.astype(BF16)
    rest = x - high.astype(F32)
    mid = rest.astype(BF16)
    return high, mid, (rest - mid.astype(F32)).astype(BF16)


def panel32(work, p, filler=lambda k: None):
    r0 = 32 * p
    diag_tile = p // 4
    lane0 = r0 % 128
    tiles = [0, 1, 2] if p < 4 else [1, 2, 3]
    rows = {ti: [work[r0 + 8 * sg:r0 + 8 * sg + 8, 128 * ti:128 * ti + 128] for sg in range(4)] for ti in tiles}
    sub_id = lax.broadcasted_iota(jnp.int32, (8, 128), 0)

    def over_lanes(u, sg):
        return jnp.broadcast_to(rows[diag_tile][sg][:, lane0 + u:lane0 + u + 1], (8, 128))

    def over_sublanes(v, i):
        return jnp.broadcast_to(v[i:i + 1, :], (8, 128))

    col, fac = {}, {}
    for u in range(16):
        for sg in range(u // 8, 4):
            col[u, sg] = over_lanes(u, sg)
    for g in range(4):
        if g < 3:
            filler(g)
        for t in range(8 * g, 8 * g + 8):
            tt = t - 8 * g
            rs = lax.rsqrt(over_sublanes(col[t, g], tt))
            for sg in range(g, 4):
                fac[t, sg] = col[t, sg] * rs
            for u in range(t + 1, min(8 * g + 16, 32)):
                ug = u // 8
                s = over_sublanes(fac[t, ug], u - 8 * ug)
                for sg in range(ug, 4):
                    col[u, sg] = col[u, sg] - fac[t, sg] * s
            for ti in tiles:
                row = over_sublanes(rows[ti][g], tt) * rs
                own = rows[ti][g] - fac[t, g] * row
                rows[ti][g] = jnp.where(sub_id > tt, own, jnp.where(sub_id == tt, row, rows[ti][g]))
                for sg in range(g + 1, 4):
                    rows[ti][sg] = rows[ti][sg] - fac[t, sg] * row
        if g < 2:
            for u in range(8 * g + 16, 8 * g + 24):
                for sg in range(u // 8, 4):
                    col[u, sg] = over_lanes(u, sg)
    for ti in tiles:
        for sg in range(4):
            work[r0 + 8 * sg:r0 + 8 * sg + 8, 128 * ti:128 * ti + 128] = rows[ti][sg]
    if p == 7:
        filler(3)
        return
    high, mid, low = split3(jnp.concatenate([jnp.concatenate(rows[ti], axis=0) for ti in tiles], axis=1))
    first = (r0 + 32 - 128 * diag_tile) // 128 * 128
    rhs = jnp.concatenate([high, mid, high, mid, low, high], axis=0)
    lhs = jnp.concatenate([high, high, mid, mid, high, low], axis=0)[:, first:256 - 128 * diag_tile]
    upd = lax.dot_general(lhs, rhs, (((0,), (0,)), ((), ())), preferred_element_type=F32)
    filler(3)
    skip = r0 + 32 - first - 128 * diag_tile
    for j, ti in enumerate(tiles):
        lanes = slice(128 * ti, 128 * ti + 128)
        work[r0 + 32:256, lanes] = work[r0 + 32:256, lanes] - upd[skip:, 128 * j:128 * j + 128]


def spread_factor(b, u_ref, x_ref, work):
    row = lax.broadcasted_iota(jnp.int32, (NB, NB), 0)
    col = lax.broadcasted_iota(jnp.int32, (NB, NB), 1)
    a, e = NB * b, NB * b + NB
    xbb = jnp.where(col <= row, work[:, NB:], 0.0)
    u_ref[a:e, a:e] = jnp.where(col >= row, work[:, :NB], 0.0)
    if b > 0:
        x_ref[a:e, :a] = dot(xbb, x_ref[a:e, :a])
        u_ref[a:e, :a] = jnp.zeros((NB, a), F32)
    x_ref[a:e, a:e] = xbb
    if b < 3:
        urow = dot(xbb, u_ref[a:e, e:])
        u_ref[a:e, e:] = urow
        for c in range(b + 1, 4):
            lo = NB * c
            uc = urow[:, lo - e:lo - e + NB]
            u_ref[lo:lo + NB, lo:] = u_ref[lo:lo + NB, lo:] - dot_tn(uc, urow[:, lo - e:])
            x_ref[lo:lo + NB, :e] = x_ref[lo:lo + NB, :e] - dot_tn(uc, x_ref[a:e, :e])


def factor_block(b, u_ref, x_ref, own_l_ref, own_diag_ref, work, filler=lambda p, k: None):
    row = lax.broadcasted_iota(jnp.int32, (NB, NB), 0)
    col = lax.broadcasted_iota(jnp.int32, (NB, NB), 1)
    at = pl.ds(pl.multiple_of(b * NB, NB), NB)
    work[:, :NB] = u_ref[at, at]
    work[:, NB:] = jnp.where(row == col, 1.0, 0.0)
    for p in range(8):
        panel32(work, p, functools.partial(filler, p))
    for n in range(4):
        pl.when(b == n)(lambda n=n: spread_factor(n, u_ref, x_ref, work))

    @pl.when(b == 3)
    def _():
        at_row, at_col = (pl.ds(pl.multiple_of(lax.axis_index(name) * NB, NB), NB) for name in ("pr", "pc"))
        own_l_ref[...] = u_ref[at_col, at_row].T
        own_diag_ref[...] = u_ref[at_row, at_row]


def factor_kernel(*refs):
    blocks, (x_ref, own_l_ref, own_diag_ref, u_ref, work) = refs[:-5], refs[-5:]
    my_col, my_row = lax.axis_index("pc"), lax.axis_index("pr")
    b = pl.program_id(0)

    @pl.when(b == 0)
    def _():
        for c in range(4):
            for r in range(4):
                at_row, at_col = (pl.ds(pl.multiple_of(v * NB, NB), NB) for v in (my_row ^ r, my_col ^ c))
                u_ref[at_row, at_col] = blocks[r % 2][c + 4 * (r // 2)]
        x_ref[...] = jnp.zeros_like(x_ref)

    factor_block(b, u_ref, x_ref, own_l_ref, own_diag_ref, work)


def call(kernel, flops, moved, vmem, **kw):
    cost = pl.CostEstimate(flops=flops, bytes_accessed=moved, transcendentals=0)
    return pl.pallas_call(kernel, cost_estimate=cost, compiler_params=pltpu.CompilerParams(vmem_limit_bytes=vmem * MIB), **kw)


def in_hbm(x):
    return pltpu.with_memory_space_constraint(x, pltpu.HBM)


def shape(*dims):
    return pltpu.HBM(dims, F32)


def near(*dims):
    return jax.ShapeDtypeStruct(dims, F32)


def factor(blocks):
    vmem = pl.BlockSpec(memory_space=pltpu.VMEM)
    return call(
        factor_kernel, 30_000_000_000, 1 << 24, 20, grid=(4,),
        out_shape=(near(SUP, SUP), shape(NB, NB), shape(NB, NB)), in_specs=[vmem] * len(blocks), out_specs=(vmem,) * 3,
        scratch_shapes=[pltpu.VMEM((SUP, SUP), F32), pltpu.VMEM((NB, 2 * NB), F32)],
    )(*blocks)


def flat_panel(panel):
    return panel.reshape(-1, 4, 2, 128).transpose(0, 2, 1, 3).reshape(-1, 128)


def dot_parts(a, b):
    total = None
    for i, j in ((2, 0), (0, 2), (1, 1), (1, 0), (0, 1), (0, 0)):
        product = lax.dot_general(a(i), b(j), (((1,), (0,)), ((), ())), preferred_element_type=F32)
        total = product if total is None else total + product
    return total


def fused_kernel(s_ref, trail_ref, l_ref, mine_ref, theirs_ref, *rest):
    x_ref, own_l_ref, own_diag_ref, out_ref, u_ref, work, u_parts, l_parts, landing, block_sem, land_sem = rest[-11:]
    b = pl.program_id(0)
    my_row = lax.axis_index("pr")

    def landing_copy(k, w):
        at = pl.ds(128 * k, 128)
        return pltpu.make_async_copy((mine_ref, theirs_ref)[w].at[at], landing.at[w, at], land_sem.at[2 * k + w])

    def block_copy(n):
        return pltpu.make_async_copy(s_ref.at[n], u_ref.at[pl.ds(n % 4 * NB, NB), pl.ds(n // 4 * NB, NB)], block_sem.at[n])

    @pl.when(b == 0)
    def _():
        half = my_row % 2
        for k in range(8):
            for w in range(2):
                landing_copy(k, w).start()
        for n in range(16):
            block_copy(n).start()
        x_ref[...] = jnp.zeros_like(x_ref)
        for k in range(8):
            for w in range(2):
                landing_copy(k, w).wait()

                def split_rows(i, carry, k=k, w=w):
                    at = pl.ds(pl.multiple_of(128 * k + 32 * i, 32), 32)
                    for n, part in enumerate(split3(landing[w, at, :])):
                        u_parts[n, at, pl.ds(pl.multiple_of((half ^ w) * SUP, SUP), SUP)] = part
                    return carry

                lax.fori_loop(0, 4, split_rows, 0)
        for n in range(16):
            block_copy(n).wait()

    for n, part in enumerate(split3(l_ref[...])):
        l_parts[n] = part

    def piece(q, k):
        deep, lanes = slice(NB * k, NB * k + NB), slice(NB * q, NB * q + NB)
        total = dot_parts(lambda i: l_parts[i, :, deep], lambda j: u_parts[j, deep, lanes])
        out_ref[:, lanes] = (trail_ref if k == 0 else out_ref)[:, lanes] - total

    factor_block(b, u_ref, x_ref, own_l_ref, own_diag_ref, work, piece)


def factor_beside(blocks, source, trail, l_rows, mine, theirs):
    rows, cols = trail.shape
    last = rows // NB - 4
    ahead = l_rows.shape[0] // NB - 4
    vmem = pl.BlockSpec(memory_space=pltpu.VMEM)
    at = pl.BlockSpec((NB, cols), lambda b: (last + b, 0))
    anywhere = pl.BlockSpec(memory_space=pl.ANY)
    operands = [in_hbm(blocks), trail if source is None else source, in_hbm(l_rows), in_hbm(mine), in_hbm(theirs)]
    specs = [anywhere, at, pl.BlockSpec((NB, SUP), lambda b: (ahead + b, 0)), anywhere, anywhere]
    if source is not None:
        operands.append(trail)
        specs.append(anywhere)
    scratch = [pltpu.VMEM((SUP, SUP), F32), pltpu.VMEM((NB, 2 * NB), F32), pltpu.VMEM((3, SUP, cols), BF16), pltpu.VMEM((3, NB, SUP), BF16),
               pltpu.VMEM((2, SUP, SUP), F32), pltpu.SemaphoreType.DMA((16,)), pltpu.SemaphoreType.DMA((16,))]
    return call(
        fused_kernel, 100_000_000_000, 1 << 25, 48, grid=(4,),
        out_shape=(near(SUP, SUP), shape(NB, NB), shape(NB, NB), shape(rows, cols)), in_specs=specs, out_specs=(vmem, vmem, vmem, at),
        scratch_shapes=scratch,
        input_output_aliases={1 if source is None else 5: 3},
    )(*operands)


def unpack_kernel(in_ref, rest_ref):
    for n, s in enumerate((3, 2, 1)):
        for half in range(2):
            rest_ref[:, NB * n + 128 * half:NB * n + 128 * half + 128] = in_ref[pl.ds(4 * half + s, NB, stride=8), :]


def unpack(panel):
    rows = panel.shape[0] - NB
    return call(
        unpack_kernel, 1_000_000, 8 * rows * SUP, 12, grid=(rows // NB,), out_shape=shape(rows, 3 * NB),
        in_specs=[pl.BlockSpec((8 * NB, 128), lambda i: (i + 1, 0))], out_specs=pl.BlockSpec((NB, 3 * NB), lambda i: (i, 0)),
    )(flat_panel(panel))


def pack_rows(i, cols, diags, out_ref):
    for s in range(4):
        def put(value, s=s):
            for half in range(2):
                out_ref[pl.ds(4 * half + s, NB, stride=8), :] = value[:, 128 * half:128 * half + 128]

        pl.when(i < s)(lambda: put(jnp.zeros((NB, NB), F32)))
        pl.when(i == s)(lambda s=s: put(diags[s][...]))
        pl.when(i > s)(lambda s=s: put(cols[s][...]))


def rows_kernel(*refs):
    (own, y, z, *far), (x_ref, out_ref, own_ref, wide) = refs[:-4], refs[-4:]
    my_col = lax.axis_index("pc")
    i = pl.program_id(0)

    def place(flip, ref):
        wide[:, pl.ds(pl.multiple_of((my_col ^ flip) * NB, NB), NB)] = ref[...]

    place(0, own)
    place(1, y)
    place(2, z)
    if len(far) == 1:
        place(3, far[0])
    else:
        pl.when(i < 2)(lambda: place(3, far[0]))
        pl.when(i >= 2)(lambda: place(3, far[1]))
    for k in range(4):
        lanes = slice(NB * k, NB * k + NB)
        part = dot_nt(wide[:, lanes], x_ref[NB * k:, lanes])
        out_ref[:, NB * k:] = part if k == 0 else out_ref[:, NB * k:] + part
    own_ref[...] = out_ref[:, pl.ds(pl.multiple_of(my_col * NB, NB), NB)]


def solve_rows(pieces, x):
    own, y, z, *far = pieces
    rows = own.shape[0]
    tile = rows // 4
    block = pl.BlockSpec((tile, NB), lambda i: (i, 0))
    far_blocks = [block] if len(far) == 1 else [
        pl.BlockSpec((tile, NB), lambda i: (jnp.minimum(i, 1), 0)), pl.BlockSpec((tile, NB), lambda i: (jnp.maximum(i - 2, 0), 0))]
    return call(
        rows_kernel, 30 * rows * SUP * SUP // 4, 12 * rows * SUP, 34, grid=(4,),
        out_shape=(shape(rows, SUP), shape(rows, NB)),
        in_specs=[block] * 3 + far_blocks + [pl.BlockSpec((SUP, SUP), lambda i: (0, 0))],
        out_specs=(pl.BlockSpec((tile, SUP), lambda i: (i, 0)), block),
        scratch_shapes=[pltpu.VMEM((tile, SUP), F32)],
    )(in_hbm(own), y, z, *far, x)


def cols_kernel(*refs):
    pieces, x_ref, outs, tall = refs[:4], refs[4], refs[5:-1], refs[-1]
    my_row = lax.axis_index("pr")
    i = pl.program_id(0)
    for j in range(4):
        tall[pl.ds(pl.multiple_of((my_row ^ j) * NB, NB), NB), :] = pieces[j][...]

    parts = [dot(x_ref[NB * k:NB * k + NB, :NB * k + NB], tall[:NB * k + NB, :]) for k in range(4)]

    def put(ref):
        for k in range(4):
            ref[NB * k:NB * k + NB, :] = parts[k]

    if len(outs) == 1:
        put(outs[0])
    else:
        pl.when(i < 4)(lambda: put(outs[0]))
        pl.when(i >= 4)(lambda: put(outs[1]))


def solve_cols(pieces, x):
    cols = pieces[0].shape[1]
    outs = [shape(SUP, min(SUP, cols))] + ([near(SUP, cols - SUP)] if cols > SUP else [])
    specs = [pl.BlockSpec((SUP, NB), lambda i: (0, jnp.minimum(i, min(SUP, cols) // NB - 1))), pl.BlockSpec((SUP, NB), lambda i: (0, jnp.maximum(i - 4, 0)))]
    return call(
        cols_kernel, 30 * cols * SUP * SUP // 4, 12 * cols * SUP, 20, grid=(cols // NB,), out_shape=outs,
        in_specs=[pl.BlockSpec((NB, NB), lambda i: (0, i))] * 4 + [pl.BlockSpec((SUP, SUP), lambda i: (0, 0))],
        out_specs=specs[:len(outs)], scratch_shapes=[pltpu.VMEM((SUP, NB), F32)],
    )(*pieces, x)


def panel_kernel(*refs):
    rest_ref, l_ref, u_ref, diag_ref, col_ref = refs[:5]
    l_parts, u_parts = refs[-2:]
    keep = rest_ref.shape[1] - NB
    i = pl.program_id(0)

    @pl.when(i == 0)
    def _():
        def split_rows(k, carry):
            at = pl.ds(pl.multiple_of(k * 64, 64), 64)
            for n, part in enumerate(split3(u_ref[at, :])):
                u_parts[n, at, :] = part
            return carry

        lax.fori_loop(0, SUP // 64, split_rows, 0)

    for n, part in enumerate(split3(l_ref[...])):
        l_parts[n] = part
    new = rest_ref[...] - dot_parts(lambda n: l_parts[n], lambda n: u_parts[n])

    @pl.when(i == 0)
    def _():
        diag_ref[...] = new[:, keep:]
        if keep:
            refs[5][...] = new[:, :keep]

    @pl.when(i > 0)
    def _():
        col_ref[...] = new[:, keep:]
        if keep:
            refs[6][...] = new[:, :keep]


def update_panel(rest, l_rows, u_panel):
    rows, width = rest.shape
    keep = width - NB
    below = lambda i: (jnp.maximum(i - 1, 0), 0)
    zero = lambda i: (0, 0)
    outs = [shape(NB, NB), shape(rows - NB, NB)] + ([shape(NB, keep), shape(rows - NB, keep)] if keep else [])
    specs = [pl.BlockSpec((NB, NB), zero), pl.BlockSpec((NB, NB), below)]
    if keep:
        specs += [pl.BlockSpec((NB, keep), zero), pl.BlockSpec((NB, keep), below)]
    return call(
        panel_kernel, 12 * rows * width * SUP, 8 * rows * width + 4 * rows * SUP, 26, grid=(rows // NB,), out_shape=outs,
        in_specs=[pl.BlockSpec((NB, width), lambda i: (i, 0)), pl.BlockSpec((NB, SUP), lambda i: (i, 0)), pl.BlockSpec((SUP, width), zero)],
        out_specs=specs, scratch_shapes=[pltpu.VMEM((3, NB, SUP), BF16), pltpu.VMEM((3, SUP, width), BF16)],
    )(in_hbm(rest), in_hbm(l_rows), u_panel)


def row_kernel(*refs):
    trail_ref, l_ref, mine_ref, theirs_ref = refs[1:5]
    keep_ref, send_ref, landing, sem = refs[-4:]
    j = pl.program_id(0)
    copies = [pltpu.make_async_copy(ref, landing.at[n], sem.at[n]) for n, ref in enumerate((mine_ref, theirs_ref))]

    @pl.when(j == 0)
    def _():
        for copy in copies:
            copy.start()
        if len(refs) == 10:
            keep_ref[:, SUP:] = refs[5][...]
            send_ref[:, SUP:] = refs[5][...]

    for n, copy in enumerate(copies):
        pl.when(j == n)(copy.wait)
    new = trail_ref[...] - dot(l_ref[...], landing[j])

    @pl.when(j == 0)
    def _():
        keep_ref[:, :SUP] = new

    @pl.when(j == 1)
    def _():
        send_ref[:, :SUP] = new


def update_row(core, trail, l_rows, mine, theirs, panel_row, step):
    extra = [] if panel_row is None else [panel_row]
    width = SUP + (0 if panel_row is None else panel_row.shape[1])
    out = pl.BlockSpec((NB, width), lambda j, h: (0, 0))
    anywhere = pl.BlockSpec(memory_space=pl.ANY)
    return call(
        row_kernel, 24 * NB * SUP * SUP, 12 * SUP * SUP, 30,
        grid_spec=pltpu.PrefetchScalarGridSpec(
            num_scalar_prefetch=1, grid=(2,),
            in_specs=[pl.BlockSpec((NB, SUP), lambda j, h: (step + 1, h[0] ^ j)), pl.BlockSpec((NB, SUP), lambda j, h: (0, 0)),
                      anywhere, anywhere] + [pl.BlockSpec(a.shape, lambda j, h: (0, 0)) for a in extra],
            out_specs=(out, out), scratch_shapes=[pltpu.VMEM((2, SUP, SUP), F32), pltpu.SemaphoreType.DMA((2,))]),
        out_shape=(shape(NB, width), shape(NB, width)),
    )(core, trail, in_hbm(l_rows), in_hbm(mine), in_hbm(theirs), *extra)


def trail_kernel(core_ref, trail_ref, l_ref, mine_ref, theirs_ref, diag_ref, *rest):
    rest, (landing, u_parts, l_parts, sem) = rest[:-4], rest[-4:]
    my_row = lax.axis_index("pr")
    j, i = pl.program_id(0), pl.program_id(1)
    copies = [pltpu.make_async_copy(ref, landing, sem.at[n]) for n, ref in enumerate((mine_ref, theirs_ref))]
    out_ref = rest[0]
    if len(rest) > 1:
        out_ref = rest[8]
        pack_rows(jnp.minimum(j * pl.num_programs(1) + i, pl.num_programs(1) + 2), rest[:4], rest[4:8], rest[9])

    @pl.when(i == 0)
    def _():
        pl.when(j == 0)(copies[0].start)
        pl.when(j == 0)(copies[0].wait)
        pl.when(j == 1)(copies[1].wait)

        def split_rows(k, carry):
            at = pl.ds(pl.multiple_of(k * 64, 64), 64)
            for n, part in enumerate(split3(landing[at, :])):
                u_parts[n, at, :] = part
            return carry

        lax.fori_loop(0, SUP // 64, split_rows, 0)
        out_ref[...] = dot_tn(diag_ref[...], landing[pl.ds(pl.multiple_of(my_row * NB, NB), NB), :])

    @pl.when(i > 0)
    def _():
        pl.when((i == 1) & (j == 0))(copies[1].start)
        for n, part in enumerate(split3(l_ref[...])):
            l_parts[n] = part
        out_ref[...] = trail_ref[...] - dot_parts(lambda n: l_parts[n], lambda n: u_parts[n])


def update_trail(core, trail, l_rows, mine, theirs, own_diag, step, out_cols=(), out_diags=()):
    rows, cols = trail.shape
    off = 1 if step < 3 else 0
    count = rows // NB - step - off - (4 if step < 3 else 0)
    at = pl.BlockSpec((NB, SUP), lambda j, i, h: (jnp.where(i == 0, step, step + off + i), h[0] ^ j))
    anywhere = pl.BlockSpec(memory_space=pl.ANY)
    ins = [at, pl.BlockSpec((NB, SUP), lambda j, i, h: (jnp.maximum(i, 1) - 1 + off, 0)), anywhere, anywhere,
           pl.BlockSpec((NB, NB), lambda j, i, h: (0, 0))]
    outs, shapes = [at], [shape(rows, cols)]
    if out_cols:
        block = lambda j, i: jnp.minimum(j * count + i, rows // NB - 1)
        ins += [pl.BlockSpec((NB, NB), lambda j, i, h, s=s: (jnp.maximum(block(j, i) - s - 1, 0), 0)) for s in range(4)]
        ins += [pl.BlockSpec((NB, NB), lambda j, i, h: (0, 0))] * 4
        outs.append(pl.BlockSpec((8 * NB, 128), lambda j, i, h: (block(j, i), 0)))
        shapes.append(shape(rows * 8, 128))
    return call(
        trail_kernel, 12 * count * NB * cols * SUP, 8 * count * NB * cols, 32,
        grid_spec=pltpu.PrefetchScalarGridSpec(num_scalar_prefetch=1, grid=(2, count), in_specs=ins, out_specs=outs, scratch_shapes=[
            pltpu.VMEM((SUP, SUP), F32), pltpu.VMEM((3, SUP, SUP), BF16), pltpu.VMEM((3, NB, SUP), BF16), pltpu.SemaphoreType.DMA((2,))]),
        out_shape=shapes, input_output_aliases={1: 0} if step else {},
    )(core, trail, in_hbm(l_rows), in_hbm(mine), in_hbm(theirs), *(in_hbm(a) for a in (own_diag, *out_cols, *out_diags)))


FLIP1 = [(0, 1), (1, 0), (2, 3), (3, 2)]
FLIP2 = [(0, 2), (2, 0), (1, 3), (3, 1)]
FLIP3 = [(0, 3), (3, 0), (1, 2), (2, 1)]


def gather_diag(block):
    have = block[None]
    for axis, perm in (("pc", FLIP1), ("pc", FLIP2), ("pr", FLIP2)):
        have = jnp.concatenate([have, lax.ppermute(have, axis, perm)], axis=0)
    return [have, lax.ppermute(have, "pr", FLIP1)]


def gather_cols(keep, send):
    return [keep, lax.ppermute(send, "pr", FLIP1), lax.ppermute(keep, "pr", FLIP2), lax.ppermute(send, "pr", FLIP3)]


def gather_all(panel):
    x = lax.ppermute(panel, "pr", FLIP2)
    other = lax.ppermute(panel, "pr", FLIP1)
    return [panel, other, x, lax.ppermute(x, "pr", FLIP1)]


def solution(mesh):
    def local_part(panel_tile, trail_tile):
        my_row = lax.axis_index("pr")
        half = my_row % 2
        core = jnp.full((1,), half, jnp.int32)
        trail = trail_tile
        out_cols, out_diags = [], []
        for step in range(4):
            if step == 0:
                diag_block, later = lax.optimization_barrier((panel_tile[:NB, 0, :], panel_tile[:NB]))
                blocks = gather_diag(diag_block)
                col_panel = panel_tile[NB:, 0, :]
                keep, send = (lax.dynamic_slice(trail_tile, (0, SUP * h), (NB, SUP)) for h in (half, 1 - half))
                panel_row = jnp.concatenate([later[:NB, s, :] for s in (3, 2, 1)], axis=1)
                rest = unpack(panel_tile)
            else:
                blocks = [lax.all_gather(diag_block, ("pc", "pr"))]
            y = lax.ppermute(col_panel, "pc", FLIP1)
            z = lax.ppermute(col_panel, "pc", FLIP2)
            col_pieces = gather_cols(keep, send)
            if step == 0:
                row_pieces = gather_all(panel_row)
            if step:
                source = trail if step == 1 else None
                trail, = update_trail(core, trail, l_rows, mine, theirs, own_diag, step - 1)
                blocks, trail = lax.optimization_barrier((blocks, trail))
            if step:
                far = [lax.ppermute(col_panel, "pc", FLIP3)]
            else:
                split = col_panel.shape[0] // 2
                far = [lax.ppermute(z[:split], "pc", FLIP1), lax.ppermute(y[split:], "pc", FLIP2)]
            if step == 0:
                x_sup, own_l, own_diag = factor(blocks)
            else:
                x_sup, own_l, own_diag, trail = factor_beside(*blocks, source, trail, l_rows, mine, theirs)
            mine, *more = solve_cols(col_pieces, x_sup)
            if step == 0:
                more = solve_cols(row_pieces, x_sup)
            theirs = lax.ppermute(mine, "pr", FLIP1)
            l_rows, own_col = solve_rows([col_panel, y, z, *far], x_sup)
            out_cols.append(own_col)
            out_diags.append(own_l)
            if step < 3:
                diag_block, col_panel, *left = update_panel(rest, l_rows, more[0])
                panel_row, rest = left if left else (None, None)
                keep, send = update_row(core, trail, l_rows, mine, theirs, panel_row, step)
        trail, flat = update_trail(core, trail, l_rows, mine, theirs, own_diag, 3, out_cols, out_diags)
        rows = trail.shape[0]
        return flat.reshape(rows, 2, 4, 128).transpose(0, 2, 1, 3).reshape(rows, 4, NB), trail

    spec_panel = P("pr", "pc", None)
    spec_trail = P("pr", "pc")
    return jax.shard_map(local_part, mesh=mesh, in_specs=(spec_panel, spec_trail), out_specs=(spec_panel, spec_trail), check_vma=False)
```

```python
import functools

import jax
import jax.numpy as jnp
from jax import lax
from jax.experimental import pallas as pl
from jax.experimental.pallas import tpu as pltpu
from jax.sharding import PartitionSpec as P


F32 = jnp.float32
BF16 = jnp.bfloat16
HIGH = lax.Precision.HIGHEST
NB = 256
SUP = 1024
MIB = 1024 * 1024


def dot(a, b):
    return lax.dot_general(a, b, (((1,), (0,)), ((), ())), precision=HIGH, preferred_element_type=F32)


def dot_nt(a, b):
    return lax.dot_general(a, b, (((1,), (1,)), ((), ())), precision=HIGH, preferred_element_type=F32)


def dot_tn(a, b):
    return lax.dot_general(a, b, (((0,), (0,)), ((), ())), precision=HIGH, preferred_element_type=F32)


def split3(x):
    high = x.astype(BF16)
    rest = x - high.astype(F32)
    mid = rest.astype(BF16)
    return high, mid, (rest - mid.astype(F32)).astype(BF16)


def panel32(work, p, filler=lambda k: None):
    r0 = 32 * p
    diag_tile = p // 4
    lane0 = r0 % 128
    tiles = [0, 1, 2] if p < 4 else [1, 2, 3]
    rows = {ti: [work[r0 + 8 * sg:r0 + 8 * sg + 8, 128 * ti:128 * ti + 128] for sg in range(4)] for ti in tiles}
    sub_id = lax.broadcasted_iota(jnp.int32, (8, 128), 0)

    def over_lanes(u, sg):
        return jnp.broadcast_to(rows[diag_tile][sg][:, lane0 + u:lane0 + u + 1], (8, 128))

    def over_sublanes(v, i):
        return jnp.broadcast_to(v[i:i + 1, :], (8, 128))

    col, fac = {}, {}
    for u in range(16):
        for sg in range(u // 8, 4):
            col[u, sg] = over_lanes(u, sg)
    for g in range(4):
        if g < 3:
            filler(g)
        for t in range(8 * g, 8 * g + 8):
            tt = t - 8 * g
            rs = lax.rsqrt(over_sublanes(col[t, g], tt))
            for sg in range(g, 4):
                fac[t, sg] = col[t, sg] * rs
            for u in range(t + 1, min(8 * g + 16, 32)):
                ug = u // 8
                s = over_sublanes(fac[t, ug], u - 8 * ug)
                for sg in range(ug, 4):
                    col[u, sg] = col[u, sg] - fac[t, sg] * s
            for ti in tiles:
                row = over_sublanes(rows[ti][g], tt) * rs
                own = rows[ti][g] - fac[t, g] * row
                rows[ti][g] = jnp.where(sub_id > tt, own, jnp.where(sub_id == tt, row, rows[ti][g]))
                for sg in range(g + 1, 4):
                    rows[ti][sg] = rows[ti][sg] - fac[t, sg] * row
        if g < 2:
            for u in range(8 * g + 16, 8 * g + 24):
                for sg in range(u // 8, 4):
                    col[u, sg] = over_lanes(u, sg)
    for ti in tiles:
        for sg in range(4):
            work[r0 + 8 * sg:r0 + 8 * sg + 8, 128 * ti:128 * ti + 128] = rows[ti][sg]
    if p == 7:
        filler(3)
        return
    high, mid, low = split3(jnp.concatenate([jnp.concatenate(rows[ti], axis=0) for ti in tiles], axis=1))
    first = (r0 + 32 - 128 * diag_tile) // 128 * 128
    rhs = jnp.concatenate([high, mid, high, mid, low, high], axis=0)
    lhs = jnp.concatenate([high, high, mid, mid, high, low], axis=0)[:, first:256 - 128 * diag_tile]
    upd = lax.dot_general(lhs, rhs, (((0,), (0,)), ((), ())), preferred_element_type=F32)
    filler(3)
    skip = r0 + 32 - first - 128 * diag_tile
    for j, ti in enumerate(tiles):
        lanes = slice(128 * ti, 128 * ti + 128)
        work[r0 + 32:256, lanes] = work[r0 + 32:256, lanes] - upd[skip:, 128 * j:128 * j + 128]


def spread_factor(b, u_ref, x_ref, work):
    row = lax.broadcasted_iota(jnp.int32, (NB, NB), 0)
    col = lax.broadcasted_iota(jnp.int32, (NB, NB), 1)
    a, e = NB * b, NB * b + NB
    xbb = jnp.where(col <= row, work[:, NB:], 0.0)
    u_ref[a:e, a:e] = jnp.where(col >= row, work[:, :NB], 0.0)
    if b > 0:
        x_ref[a:e, :a] = dot(xbb, x_ref[a:e, :a])
        u_ref[a:e, :a] = jnp.zeros((NB, a), F32)
    x_ref[a:e, a:e] = xbb
    if b < 3:
        urow = dot(xbb, u_ref[a:e, e:])
        u_ref[a:e, e:] = urow
        for c in range(b + 1, 4):
            lo = NB * c
            uc = urow[:, lo - e:lo - e + NB]
            u_ref[lo:lo + NB, lo:] = u_ref[lo:lo + NB, lo:] - dot_tn(uc, urow[:, lo - e:])
            x_ref[lo:lo + NB, :e] = x_ref[lo:lo + NB, :e] - dot_tn(uc, x_ref[a:e, :e])


def factor_block(b, u_ref, x_ref, own_l_ref, own_diag_ref, work, filler=lambda p, k: None):
    row = lax.broadcasted_iota(jnp.int32, (NB, NB), 0)
    col = lax.broadcasted_iota(jnp.int32, (NB, NB), 1)
    at = pl.ds(pl.multiple_of(b * NB, NB), NB)
    work[:, :NB] = u_ref[at, at]
    work[:, NB:] = jnp.where(row == col, 1.0, 0.0)
    for p in range(8):
        panel32(work, p, functools.partial(filler, p))
    for n in range(4):
        pl.when(b == n)(lambda n=n: spread_factor(n, u_ref, x_ref, work))

    @pl.when(b == 3)
    def _():
        at_row, at_col = (pl.ds(pl.multiple_of(lax.axis_index(name) * NB, NB), NB) for name in ("pr", "pc"))
        own_l_ref[...] = u_ref[at_col, at_row].T
        own_diag_ref[...] = u_ref[at_row, at_row]


def factor_kernel(*refs):
    blocks, (x_ref, own_l_ref, own_diag_ref, u_ref, work) = refs[:-5], refs[-5:]
    my_col, my_row = lax.axis_index("pc"), lax.axis_index("pr")
    b = pl.program_id(0)

    @pl.when(b == 0)
    def _():
        for c in range(4):
            for r in range(4):
                at_row, at_col = (pl.ds(pl.multiple_of(v * NB, NB), NB) for v in (my_row ^ r, my_col ^ c))
                u_ref[at_row, at_col] = blocks[r % 2][c + 4 * (r // 2)]
        x_ref[...] = jnp.zeros_like(x_ref)

    factor_block(b, u_ref, x_ref, own_l_ref, own_diag_ref, work)


def call(kernel, flops, moved, vmem, **kw):
    cost = pl.CostEstimate(flops=flops, bytes_accessed=moved, transcendentals=0)
    return pl.pallas_call(kernel, cost_estimate=cost, compiler_params=pltpu.CompilerParams(vmem_limit_bytes=vmem * MIB), **kw)


def in_hbm(x):
    return pltpu.with_memory_space_constraint(x, pltpu.HBM)


def shape(*dims):
    return pltpu.HBM(dims, F32)


def near(*dims):
    return jax.ShapeDtypeStruct(dims, F32)


def factor(blocks):
    vmem = pl.BlockSpec(memory_space=pltpu.VMEM)
    return call(
        factor_kernel, 30_000_000_000, 1 << 24, 20, grid=(4,),
        out_shape=(near(SUP, SUP), shape(NB, NB), shape(NB, NB)), in_specs=[vmem] * len(blocks), out_specs=(vmem,) * 3,
        scratch_shapes=[pltpu.VMEM((SUP, SUP), F32), pltpu.VMEM((NB, 2 * NB), F32)],
    )(*blocks)


def flat_panel(panel):
    return panel.reshape(-1, 4, 2, 128).transpose(0, 2, 1, 3).reshape(-1, 128)


def dot_parts(a, b):
    total = None
    for i, j in ((2, 0), (0, 2), (1, 1), (1, 0), (0, 1), (0, 0)):
        product = lax.dot_general(a(i), b(j), (((1,), (0,)), ((), ())), preferred_element_type=F32)
        total = product if total is None else total + product
    return total


def fused_kernel(s_ref, trail_ref, l_ref, mine_ref, theirs_ref, *rest):
    x_ref, own_l_ref, own_diag_ref, out_ref, u_ref, work, u_parts, l_parts, landing, block_sem, land_sem = rest[-11:]
    b = pl.program_id(0)
    my_row = lax.axis_index("pr")

    def landing_copy(k, w):
        at = pl.ds(128 * k, 128)
        return pltpu.make_async_copy((mine_ref, theirs_ref)[w].at[at], landing.at[w, at], land_sem.at[2 * k + w])

    def block_copy(n):
        return pltpu.make_async_copy(s_ref.at[n], u_ref.at[pl.ds(n % 4 * NB, NB), pl.ds(n // 4 * NB, NB)], block_sem.at[n])

    @pl.when(b == 0)
    def _():
        half = my_row % 2
        for k in range(8):
            for w in range(2):
                landing_copy(k, w).start()
        for n in range(16):
            block_copy(n).start()
        x_ref[...] = jnp.zeros_like(x_ref)
        for k in range(8):
            for w in range(2):
                landing_copy(k, w).wait()

                def split_rows(i, carry, k=k, w=w):
                    at = pl.ds(pl.multiple_of(128 * k + 32 * i, 32), 32)
                    for n, part in enumerate(split3(landing[w, at, :])):
                        u_parts[n, at, pl.ds(pl.multiple_of((half ^ w) * SUP, SUP), SUP)] = part
                    return carry

                lax.fori_loop(0, 4, split_rows, 0)
        for n in range(16):
            block_copy(n).wait()

    for n, part in enumerate(split3(l_ref[...])):
        l_parts[n] = part

    def piece(q, k):
        deep, lanes = slice(NB * k, NB * k + NB), slice(NB * q, NB * q + NB)
        total = dot_parts(lambda i: l_parts[i, :, deep], lambda j: u_parts[j, deep, lanes])
        out_ref[:, lanes] = (trail_ref if k == 0 else out_ref)[:, lanes] - total

    factor_block(b, u_ref, x_ref, own_l_ref, own_diag_ref, work, piece)


def factor_beside(blocks, source, trail, l_rows, mine, theirs):
    rows, cols = trail.shape
    last = rows // NB - 4
    ahead = l_rows.shape[0] // NB - 4
    vmem = pl.BlockSpec(memory_space=pltpu.VMEM)
    at = pl.BlockSpec((NB, cols), lambda b: (last + b, 0))
    anywhere = pl.BlockSpec(memory_space=pl.ANY)
    operands = [in_hbm(blocks), trail if source is None else source, in_hbm(l_rows), in_hbm(mine), in_hbm(theirs)]
    specs = [anywhere, at, pl.BlockSpec((NB, SUP), lambda b: (ahead + b, 0)), anywhere, anywhere]
    if source is not None:
        operands.append(trail)
        specs.append(anywhere)
    scratch = [pltpu.VMEM((SUP, SUP), F32), pltpu.VMEM((NB, 2 * NB), F32), pltpu.VMEM((3, SUP, cols), BF16), pltpu.VMEM((3, NB, SUP), BF16),
               pltpu.VMEM((2, SUP, SUP), F32), pltpu.SemaphoreType.DMA((16,)), pltpu.SemaphoreType.DMA((16,))]
    return call(
        fused_kernel, 100_000_000_000, 1 << 25, 48, grid=(4,),
        out_shape=(near(SUP, SUP), shape(NB, NB), shape(NB, NB), shape(rows, cols)), in_specs=specs, out_specs=(vmem, vmem, vmem, at),
        scratch_shapes=scratch,
        input_output_aliases={1 if source is None else 5: 3},
    )(*operands)


def unpack_kernel(in_ref, rest_ref):
    for n, s in enumerate((3, 2, 1)):
        for half in range(2):
            rest_ref[:, NB * n + 128 * half:NB * n + 128 * half + 128] = in_ref[pl.ds(4 * half + s, NB, stride=8), :]


def unpack(panel):
    rows = panel.shape[0] - NB
    return call(
        unpack_kernel, 1_000_000, 8 * rows * SUP, 12, grid=(rows // NB,), out_shape=shape(rows, 3 * NB),
        in_specs=[pl.BlockSpec((8 * NB, 128), lambda i: (i + 1, 0))], out_specs=pl.BlockSpec((NB, 3 * NB), lambda i: (i, 0)),
    )(flat_panel(panel))


def pack_rows(n, cols, diags, out_ref):
    for s in range(4):
        value = jnp.where(n > s, cols[s][...], jnp.where(n == s, diags[s][...], 0.0))
        for half in range(2):
            out_ref[pl.ds(4 * half + s, NB, stride=8), :] = value[:, 128 * half:128 * half + 128]


def rows_kernel(*refs):
    (own, y, z, *far), (x_ref, out_ref, own_ref, wide) = refs[:-4], refs[-4:]
    my_col = lax.axis_index("pc")
    i = pl.program_id(0)

    def place(flip, ref):
        wide[:, pl.ds(pl.multiple_of((my_col ^ flip) * NB, NB), NB)] = ref[...]

    place(0, own)
    place(1, y)
    place(2, z)
    if len(far) == 1:
        place(3, far[0])
    else:
        pl.when(i < 2)(lambda: place(3, far[0]))
        pl.when(i >= 2)(lambda: place(3, far[1]))
    for k in range(4):
        lanes = slice(NB * k, NB * k + NB)
        part = dot_nt(wide[:, lanes], x_ref[NB * k:, lanes])
        out_ref[:, NB * k:] = part if k == 0 else out_ref[:, NB * k:] + part
    own_ref[...] = out_ref[:, pl.ds(pl.multiple_of(my_col * NB, NB), NB)]


def solve_rows(pieces, x):
    own, y, z, *far = pieces
    rows = own.shape[0]
    tile = rows // 4
    block = pl.BlockSpec((tile, NB), lambda i: (i, 0))
    far_blocks = [block] if len(far) == 1 else [
        pl.BlockSpec((tile, NB), lambda i: (jnp.minimum(i, 1), 0)), pl.BlockSpec((tile, NB), lambda i: (jnp.maximum(i - 2, 0), 0))]
    return call(
        rows_kernel, 30 * rows * SUP * SUP // 4, 12 * rows * SUP, 34, grid=(4,),
        out_shape=(shape(rows, SUP), shape(rows, NB)),
        in_specs=[block] * 3 + far_blocks + [pl.BlockSpec((SUP, SUP), lambda i: (0, 0))],
        out_specs=(pl.BlockSpec((tile, SUP), lambda i: (i, 0)), block),
        scratch_shapes=[pltpu.VMEM((tile, SUP), F32)],
    )(in_hbm(own), y, z, *far, x)


def cols_kernel(*refs):
    pieces, x_ref, outs, tall, done = refs[:4], refs[4], refs[5:-2], refs[-2], refs[-1]
    my_row = lax.axis_index("pr")
    i = pl.program_id(0)
    for j in range(4):
        tall[pl.ds(pl.multiple_of((my_row ^ j) * NB, NB), NB), :] = pieces[j][...]

    for k in range(4):
        at = slice(NB * k, NB * k + NB)
        part = dot(x_ref[NB * k:, at], tall[at, :])
        done[NB * k:, :] = part if k == 0 else done[NB * k:, :] + part

    def put(ref):
        ref[...] = done[...]

    if len(outs) == 1:
        put(outs[0])
    else:
        pl.when(i < 4)(lambda: put(outs[0]))
        pl.when(i >= 4)(lambda: put(outs[1]))


def solve_cols(pieces, x):
    cols = pieces[0].shape[1]
    outs = [shape(SUP, min(SUP, cols))] + ([near(SUP, cols - SUP)] if cols > SUP else [])
    specs = [pl.BlockSpec((SUP, NB), lambda i: (0, jnp.minimum(i, min(SUP, cols) // NB - 1))), pl.BlockSpec((SUP, NB), lambda i: (0, jnp.maximum(i - 4, 0)))]
    return call(
        cols_kernel, 30 * cols * SUP * SUP // 4, 12 * cols * SUP, 20, grid=(cols // NB,), out_shape=outs,
        in_specs=[pl.BlockSpec((NB, NB), lambda i: (0, i))] * 4 + [pl.BlockSpec((SUP, SUP), lambda i: (0, 0))],
        out_specs=specs[:len(outs)], scratch_shapes=[pltpu.VMEM((SUP, NB), F32), pltpu.VMEM((SUP, NB), F32)],
    )(*pieces, x)


def panel_kernel(*refs):
    rest_ref, l_ref, u_ref, diag_ref, col_ref = refs[:5]
    l_parts, u_parts = refs[-2:]
    keep = rest_ref.shape[1] - NB
    i = pl.program_id(0)

    @pl.when(i == 0)
    def _():
        def split_rows(k, carry):
            at = pl.ds(pl.multiple_of(k * 64, 64), 64)
            for n, part in enumerate(split3(u_ref[at, :])):
                u_parts[n, at, :] = part
            return carry

        lax.fori_loop(0, SUP // 64, split_rows, 0)

    for n, part in enumerate(split3(l_ref[...])):
        l_parts[n] = part
    new = rest_ref[...] - dot_parts(lambda n: l_parts[n], lambda n: u_parts[n])

    @pl.when(i == 0)
    def _():
        diag_ref[...] = new[:, keep:]
        if keep:
            refs[5][...] = new[:, :keep]

    @pl.when(i > 0)
    def _():
        col_ref[...] = new[:, keep:]
        if keep:
            refs[6][...] = new[:, :keep]


def update_panel(rest, l_rows, u_panel):
    rows, width = rest.shape
    keep = width - NB
    below = lambda i: (jnp.maximum(i - 1, 0), 0)
    zero = lambda i: (0, 0)
    outs = [shape(NB, NB), shape(rows - NB, NB)] + ([shape(NB, keep), shape(rows - NB, keep)] if keep else [])
    specs = [pl.BlockSpec((NB, NB), zero), pl.BlockSpec((NB, NB), below)]
    if keep:
        specs += [pl.BlockSpec((NB, keep), zero), pl.BlockSpec((NB, keep), below)]
    return call(
        panel_kernel, 12 * rows * width * SUP, 8 * rows * width + 4 * rows * SUP, 26, grid=(rows // NB,), out_shape=outs,
        in_specs=[pl.BlockSpec((NB, width), lambda i: (i, 0)), pl.BlockSpec((NB, SUP), lambda i: (i, 0)), pl.BlockSpec((SUP, width), zero)],
        out_specs=specs, scratch_shapes=[pltpu.VMEM((3, NB, SUP), BF16), pltpu.VMEM((3, SUP, width), BF16)],
    )(in_hbm(rest), in_hbm(l_rows), u_panel)


def row_kernel(*refs):
    trail_ref, l_ref, mine_ref, theirs_ref = refs[1:5]
    keep_ref, send_ref = refs[-2:]
    j = pl.program_id(0)
    lanes = pl.ds(pl.multiple_of(j % 2 * (SUP // 2), SUP // 2), SUP // 2)

    @pl.when(j < 2)
    def _():
        keep_ref[:, lanes] = trail_ref[...] - dot(l_ref[...], mine_ref[...])
        if len(refs) == 8:
            keep_ref[:, SUP:] = refs[5][...]
            send_ref[:, SUP:] = refs[5][...]

    @pl.when(j >= 2)
    def _():
        send_ref[:, lanes] = trail_ref[...] - dot(l_ref[...], theirs_ref[...])


def update_row(core, trail, l_rows, mine, theirs, panel_row, step):
    extra = [] if panel_row is None else [panel_row]
    width = SUP + (0 if panel_row is None else panel_row.shape[1])
    out = pl.BlockSpec((NB, width), lambda j, h: (0, 0))
    return call(
        row_kernel, 24 * NB * SUP * SUP, 12 * SUP * SUP, 30,
        grid_spec=pltpu.PrefetchScalarGridSpec(
            num_scalar_prefetch=1, grid=(4,),
            in_specs=[pl.BlockSpec((NB, SUP // 2), lambda j, h: (step + 1, 2 * (h[0] ^ (j // 2)) + j % 2)), pl.BlockSpec((NB, SUP), lambda j, h: (0, 0)),
                      pl.BlockSpec((SUP, SUP // 2), lambda j, h: (0, jnp.minimum(j, 1))), pl.BlockSpec((SUP, SUP // 2), lambda j, h: (0, jnp.maximum(j - 2, 0)))]
            + [pl.BlockSpec(a.shape, lambda j, h: (0, 0)) for a in extra],
            out_specs=(out, out)),
        out_shape=(shape(NB, width), shape(NB, width)),
    )(core, trail, in_hbm(l_rows), in_hbm(mine), in_hbm(theirs), *extra)


def trail_kernel(core_ref, trail_ref, l_ref, mine_ref, theirs_ref, diag_ref, *rest):
    rest, (landing, u_parts, l_parts, sem) = rest[:-4], rest[-4:]
    my_row = lax.axis_index("pr")
    j, i = pl.program_id(0), pl.program_id(1)
    quarter = SUP // 4
    first = [pltpu.make_async_copy(mine_ref.at[at], landing.at[at], sem.at[n]) for n, at in enumerate(pl.ds(n * quarter, quarter) for n in range(4))]
    second = pltpu.make_async_copy(theirs_ref, landing, sem.at[4])
    out_ref = rest[8] if len(rest) > 1 else rest[0]

    @pl.when(i == 0)
    def _():
        for copy in first:
            pl.when(j == 0)(copy.start)
        pl.when(j == 1)(second.wait)
        for n, copy in enumerate(first):
            pl.when(j == 0)(copy.wait)

            def split_rows(k, carry, n=n):
                at = pl.ds(pl.multiple_of(n * quarter + k * 64, 64), 64)
                for m, part in enumerate(split3(landing[at, :])):
                    u_parts[m, at, :] = part
                return carry

            lax.fori_loop(0, quarter // 64, split_rows, 0)
        out_ref[...] = dot_tn(diag_ref[...], landing[pl.ds(pl.multiple_of(my_row * NB, NB), NB), :])

    @pl.when(i > 0)
    def _():
        pl.when((i == 1) & (j == 0))(second.start)
        for n, part in enumerate(split3(l_ref[...])):
            l_parts[n] = part
        out_ref[...] = trail_ref[...] - dot_parts(lambda n: l_parts[n], lambda n: u_parts[n])
        if len(rest) > 1:
            count = pl.num_programs(1)
            pack_rows(jnp.minimum(j * (count - 1) + i - 1, count + 2), rest[:4], rest[4:8], rest[9])


def update_trail(core, trail, l_rows, mine, theirs, own_diag, step, out_cols=(), out_diags=()):
    rows, cols = trail.shape
    off = 1 if step < 3 else 0
    count = rows // NB - step - off - (4 if step < 3 else 0)
    at = pl.BlockSpec((NB, SUP), lambda j, i, h: (jnp.where(i == 0, step, step + off + i), h[0] ^ j))
    anywhere = pl.BlockSpec(memory_space=pl.ANY)
    ins = [at, pl.BlockSpec((NB, SUP), lambda j, i, h: (jnp.maximum(i, 1) - 1 + off, 0)), anywhere, anywhere,
           pl.BlockSpec((NB, NB), lambda j, i, h: (0, 0))]
    outs, shapes = [at], [shape(rows, cols)]
    if out_cols:
        block = lambda j, i: jnp.clip(j * (count - 1) + i - 1, 0, rows // NB - 1)
        ins += [pl.BlockSpec((NB, NB), lambda j, i, h, s=s: (jnp.maximum(block(j, i) - s - 1, 0), 0)) for s in range(4)]
        ins += [pl.BlockSpec((NB, NB), lambda j, i, h: (0, 0))] * 4
        outs.append(pl.BlockSpec((8 * NB, 128), lambda j, i, h: (block(j, i), 0)))
        shapes.append(shape(rows * 8, 128))
    return call(
        trail_kernel, 12 * count * NB * cols * SUP, 8 * count * NB * cols, 32,
        grid_spec=pltpu.PrefetchScalarGridSpec(num_scalar_prefetch=1, grid=(2, count), in_specs=ins, out_specs=outs, scratch_shapes=[
            pltpu.VMEM((SUP, SUP), F32), pltpu.VMEM((3, SUP, SUP), BF16), pltpu.VMEM((3, NB, SUP), BF16), pltpu.SemaphoreType.DMA((5,))]),
        out_shape=shapes, input_output_aliases={1: 0} if step else {},
    )(core, trail, in_hbm(l_rows), in_hbm(mine), in_hbm(theirs), *(in_hbm(a) for a in (own_diag, *out_cols, *out_diags)))


FLIP1 = [(0, 1), (1, 0), (2, 3), (3, 2)]
FLIP2 = [(0, 2), (2, 0), (1, 3), (3, 1)]
FLIP3 = [(0, 3), (3, 0), (1, 2), (2, 1)]


def gather_diag(block):
    y = functools.partial(lax.ppermute, axis_name="pc", perm=FLIP1)
    z = functools.partial(lax.ppermute, axis_name="pc", perm=FLIP2)
    x = functools.partial(lax.ppermute, axis_name="pr", perm=FLIP2)
    at_y, at_z, at_x = y(block), z(block), x(block)
    at_yz, at_xy, at_xz = z(at_y), x(at_y), x(at_z)
    at_xyz = x(at_yz)
    have = jnp.stack([block, at_y, at_z, at_yz, at_x, at_xy, at_xz, at_xyz])
    return [have, lax.ppermute(have, "pr", FLIP1)]


def gather_cols(keep, send):
    return [keep, lax.ppermute(send, "pr", FLIP1), lax.ppermute(keep, "pr", FLIP2), lax.ppermute(send, "pr", FLIP3)]


def gather_all(panel):
    x = lax.ppermute(panel, "pr", FLIP2)
    other = lax.ppermute(panel, "pr", FLIP1)
    return [panel, other, x, lax.ppermute(x, "pr", FLIP1)]


def solution(mesh):
    def local_part(panel_tile, trail_tile):
        my_row = lax.axis_index("pr")
        half = my_row % 2
        core = jnp.full((1,), half, jnp.int32)
        trail = trail_tile
        out_cols, out_diags = [], []
        for step in range(4):
            if step == 0:
                diag_block, later = lax.optimization_barrier((panel_tile[:NB, 0, :], panel_tile[:NB]))
                blocks = gather_diag(diag_block)
                col_panel = panel_tile[NB:, 0, :]
                keep, send = (lax.dynamic_slice(trail_tile, (0, SUP * h), (NB, SUP)) for h in (half, 1 - half))
                panel_row = jnp.concatenate([later[:NB, s, :] for s in (3, 2, 1)], axis=1)
                rest = unpack(panel_tile)
            else:
                blocks = [lax.all_gather(diag_block, ("pc", "pr"))]
            y = lax.ppermute(col_panel, "pc", FLIP1)
            z = lax.ppermute(col_panel, "pc", FLIP2)
            col_pieces = gather_cols(keep, send)
            if step == 0:
                row_pieces = gather_all(panel_row)
            if step:
                source = trail if step == 1 else None
                trail, = update_trail(core, trail, l_rows, mine, theirs, own_diag, step - 1)
                blocks, trail = lax.optimization_barrier((blocks, trail))
            if step:
                far = [lax.ppermute(col_panel, "pc", FLIP3)]
            else:
                split = col_panel.shape[0] // 2
                far = [lax.ppermute(z[:split], "pc", FLIP1), lax.ppermute(y[split:], "pc", FLIP2)]
            if step == 0:
                x_sup, own_l, own_diag = factor(blocks)
            else:
                x_sup, own_l, own_diag, trail = factor_beside(*blocks, source, trail, l_rows, mine, theirs)
            mine, *more = solve_cols(col_pieces, x_sup)
            if step == 0:
                more = solve_cols(row_pieces, x_sup)
            theirs = lax.ppermute(mine, "pr", FLIP1)
            l_rows, own_col = solve_rows([col_panel, y, z, *far], x_sup)
            out_cols.append(own_col)
            out_diags.append(own_l)
            if step < 3:
                diag_block, col_panel, *left = update_panel(rest, l_rows, more[0])
                panel_row, rest = left if left else (None, None)
                keep, send = update_row(core, trail, l_rows, mine, theirs, panel_row, step)
        trail, flat = update_trail(core, trail, l_rows, mine, theirs, own_diag, 3, out_cols, out_diags)
        rows = trail.shape[0]
        return flat.reshape(rows, 2, 4, 128).transpose(0, 2, 1, 3).reshape(rows, 4, NB), trail

    spec_panel = P("pr", "pc", None)
    spec_trail = P("pr", "pc")
    return jax.shard_map(local_part, mesh=mesh, in_specs=(spec_panel, spec_trail), out_specs=(spec_panel, spec_trail), check_vma=False)
```

```python
import functools

import jax
import jax.numpy as jnp
from jax import lax
from jax.experimental import pallas as pl
from jax.experimental.pallas import tpu as pltpu
from jax.sharding import PartitionSpec as P


F32 = jnp.float32
BF16 = jnp.bfloat16
HIGH = lax.Precision.HIGHEST
NB = 256
LANES = 128
SUP = 1024
MIB = 1024 * 1024


def dot(a, b):
    return lax.dot_general(a, b, (((1,), (0,)), ((), ())), precision=HIGH, preferred_element_type=F32)


def dot_nt(a, b):
    return lax.dot_general(a, b, (((1,), (1,)), ((), ())), precision=HIGH, preferred_element_type=F32)


def dot_tn(a, b):
    return lax.dot_general(a, b, (((0,), (0,)), ((), ())), precision=HIGH, preferred_element_type=F32)


def split3(x):
    high = x.astype(BF16)
    rest = x - high.astype(F32)
    mid = rest.astype(BF16)
    return high, mid, (rest - mid.astype(F32)).astype(BF16)


def panel32(work, p, filler=lambda: None):
    r0 = 32 * p
    diag_tile = p // 4
    lane0 = r0 % LANES
    tiles = [0, 1, 2] if p < 4 else [1, 2, 3]
    rows = {ti: [work[r0 + 8 * sg:r0 + 8 * sg + 8, LANES * ti:LANES * ti + LANES] for sg in range(4)] for ti in tiles}
    sub_id = lax.broadcasted_iota(jnp.int32, (8, LANES), 0)

    def over_lanes(u, sg):
        return jnp.broadcast_to(rows[diag_tile][sg][:, lane0 + u:lane0 + u + 1], (8, LANES))

    def over_sublanes(v, i):
        return jnp.broadcast_to(v[i:i + 1, :], (8, LANES))

    col, fac = {}, {}
    for u in range(16):
        for sg in range(u // 8, 4):
            col[u, sg] = over_lanes(u, sg)
    filler()
    for g in range(4):
        for t in range(8 * g, 8 * g + 8):
            tt = t - 8 * g
            rs = lax.rsqrt(over_sublanes(col[t, g], tt))
            for sg in range(g, 4):
                fac[t, sg] = col[t, sg] * rs
            for u in range(t + 1, min(8 * g + 16, 32)):
                ug = u // 8
                s = over_sublanes(col[t, ug], u - 8 * ug) * rs if u == t + 1 else over_sublanes(fac[t, ug], u - 8 * ug)
                for sg in range(ug, 4):
                    col[u, sg] = col[u, sg] - fac[t, sg] * s
            for ti in tiles:
                row = over_sublanes(rows[ti][g], tt) * rs
                own = rows[ti][g] - fac[t, g] * row
                rows[ti][g] = jnp.where(sub_id > tt, own, jnp.where(sub_id == tt, row, rows[ti][g]))
                for sg in range(g + 1, 4):
                    rows[ti][sg] = rows[ti][sg] - fac[t, sg] * row
        if g < 2:
            for u in range(8 * g + 16, 8 * g + 24):
                for sg in range(u // 8, 4):
                    col[u, sg] = over_lanes(u, sg)
    for ti in tiles:
        for sg in range(4):
            work[r0 + 8 * sg:r0 + 8 * sg + 8, LANES * ti:LANES * ti + LANES] = rows[ti][sg]
    if p == 7:
        return
    high, mid, low = split3(jnp.concatenate([jnp.concatenate(rows[ti], axis=0) for ti in tiles], axis=1))
    first = (r0 + 32 - LANES * diag_tile) // LANES * LANES
    rhs = jnp.concatenate([high, mid, high, mid, low, high], axis=0)
    lhs = jnp.concatenate([high, high, mid, mid, high, low], axis=0)[:, first:256 - LANES * diag_tile]
    upd = lax.dot_general(lhs, rhs, (((0,), (0,)), ((), ())), preferred_element_type=F32)
    skip = r0 + 32 - first - LANES * diag_tile
    for j, ti in enumerate(tiles):
        lanes = slice(LANES * ti, LANES * ti + LANES)
        work[r0 + 32:256, lanes] = work[r0 + 32:256, lanes] - upd[skip:, LANES * j:LANES * j + LANES]


def spread_factor(b, u_ref, x_ref, work):
    row = lax.broadcasted_iota(jnp.int32, (NB, NB), 0)
    col = lax.broadcasted_iota(jnp.int32, (NB, NB), 1)
    a, e = NB * b, NB * b + NB
    xbb = jnp.where(col <= row, work[:, NB:], 0.0)
    u_ref[a:e, a:e] = jnp.where(col >= row, work[:, :NB], 0.0)
    if b > 0:
        x_ref[a:e, :a] = dot(xbb, x_ref[a:e, :a])
        u_ref[a:e, :a] = jnp.zeros((NB, a), F32)
    x_ref[a:e, a:e] = xbb
    if b < 3:
        urow = dot(xbb, u_ref[a:e, e:])
        u_ref[a:e, e:] = urow
        for c in range(b + 1, 4):
            lo = NB * c
            uc = urow[:, lo - e:lo - e + NB]
            u_ref[lo:lo + NB, lo:] = u_ref[lo:lo + NB, lo:] - dot_tn(uc, urow[:, lo - e:])
            x_ref[lo:lo + NB, :e] = x_ref[lo:lo + NB, :e] - dot_tn(uc, x_ref[a:e, :e])


def factor_block(b, u_ref, x_ref, own_l_ref, own_diag_ref, work, filler=lambda p: None):
    row = lax.broadcasted_iota(jnp.int32, (NB, NB), 0)
    col = lax.broadcasted_iota(jnp.int32, (NB, NB), 1)
    at = pl.ds(pl.multiple_of(b * NB, NB), NB)
    work[:, :NB] = u_ref[at, at]
    work[:, NB:] = jnp.where(row == col, 1.0, 0.0)
    for p in range(8):
        panel32(work, p, functools.partial(filler, p))
    for n in range(4):
        pl.when(b == n)(lambda n=n: spread_factor(n, u_ref, x_ref, work))

    @pl.when(b == 3)
    def _():
        at_row, at_col = (pl.ds(pl.multiple_of(lax.axis_index(name) * NB, NB), NB) for name in ("pr", "pc"))
        own_l_ref[...] = u_ref[at_col, at_row].T
        own_diag_ref[...] = u_ref[at_row, at_row]


def factor_kernel(*refs):
    blocks, (x_ref, own_l_ref, own_diag_ref, u_ref, work) = refs[:-5], refs[-5:]
    my_col, my_row = lax.axis_index("pc"), lax.axis_index("pr")
    b = pl.program_id(0)

    @pl.when(b == 0)
    def _():
        for c in range(4):
            for r in range(4):
                at_row, at_col = (pl.ds(pl.multiple_of(v * NB, NB), NB) for v in (my_row ^ r, my_col ^ c))
                u_ref[at_row, at_col] = blocks[r % 2][c + 4 * (r // 2)]
        x_ref[...] = jnp.zeros_like(x_ref)

    factor_block(b, u_ref, x_ref, own_l_ref, own_diag_ref, work)


def call(kernel, flops, moved, vmem, **kw):
    cost = pl.CostEstimate(flops=flops, bytes_accessed=moved, transcendentals=0)
    return pl.pallas_call(kernel, cost_estimate=cost, compiler_params=pltpu.CompilerParams(vmem_limit_bytes=vmem * MIB), **kw)


def fixed(*dims):
    return pl.BlockSpec(dims, lambda *ids: (0,) * len(dims))


def in_hbm(x):
    return pltpu.with_memory_space_constraint(x, pltpu.HBM)


def shape(*dims):
    return pltpu.HBM(dims, F32)


def near(*dims):
    return jax.ShapeDtypeStruct(dims, F32)


def factor(blocks):
    vmem = pl.BlockSpec(memory_space=pltpu.VMEM)
    return call(
        factor_kernel, 30_000_000_000, 1 << 24, 20, grid=(4,),
        out_shape=(near(SUP, SUP), shape(NB, NB), shape(NB, NB)), in_specs=[vmem] * len(blocks), out_specs=(vmem,) * 3,
        scratch_shapes=[pltpu.VMEM((SUP, SUP), F32), pltpu.VMEM((NB, 2 * NB), F32)],
    )(*blocks)


def flat_panel(panel):
    return panel.reshape(-1, 4, 2, LANES).transpose(0, 2, 1, 3).reshape(-1, LANES)


def dot_parts(a, b):
    total = None
    for i, j in ((2, 0), (0, 2), (1, 1), (1, 0), (0, 1), (0, 0)):
        product = lax.dot_general(a(i), b(j), (((1,), (0,)), ((), ())), preferred_element_type=F32)
        total = product if total is None else total + product
    return total


def fused_kernel(s_ref, trail_ref, l_ref, mine_ref, theirs_ref, *rest):
    x_ref, own_l_ref, own_diag_ref, out_ref, u_ref, work, u_parts, l_parts, landing, block_sem, land_sem = rest[-11:]
    b = pl.program_id(0)
    my_row = lax.axis_index("pr")

    def landing_copy(k, w):
        at = pl.ds(LANES * k, LANES)
        return pltpu.make_async_copy((mine_ref, theirs_ref)[w].at[at], landing.at[w, at], land_sem.at[2 * k + w])

    def block_copy(n):
        return pltpu.make_async_copy(s_ref.at[n], u_ref.at[pl.ds(n % 4 * NB, NB), pl.ds(n // 4 * NB, NB)], block_sem.at[n])

    @pl.when(b == 0)
    def _():
        half = my_row % 2
        for k in range(8):
            for w in range(2):
                landing_copy(k, w).start()
        for n in range(16):
            block_copy(n).start()
        x_ref[...] = jnp.zeros_like(x_ref)
        for k in range(8):
            for w in range(2):
                landing_copy(k, w).wait()

                def split_rows(i, carry, k=k, w=w):
                    at = pl.ds(pl.multiple_of(LANES * k + 32 * i, 32), 32)
                    for n, part in enumerate(split3(landing[w, at, :])):
                        u_parts[n, at, pl.ds(pl.multiple_of((half ^ w) * SUP, SUP), SUP)] = part
                    return carry

                lax.fori_loop(0, 4, split_rows, 0)
        for n in range(16):
            block_copy(n).wait()

    for n, part in enumerate(split3(l_ref[...])):
        l_parts[n] = part

    def beside(q):
        lanes = slice(NB * q, NB * q + NB)
        for k in range(4):
            deep = slice(NB * k, NB * k + NB)
            total = dot_parts(lambda i: l_parts[i, :, deep], lambda j: u_parts[j, deep, lanes])
            out_ref[:, lanes] = (trail_ref if k == 0 else out_ref)[:, lanes] - total

    factor_block(b, u_ref, x_ref, own_l_ref, own_diag_ref, work, beside)


def factor_beside(blocks, source, trail, l_rows, mine, theirs):
    rows, cols = trail.shape
    last = rows // NB - 4
    ahead = l_rows.shape[0] // NB - 4
    vmem = pl.BlockSpec(memory_space=pltpu.VMEM)
    at = pl.BlockSpec((NB, cols), lambda b: (last + b, 0))
    anywhere = pl.BlockSpec(memory_space=pl.ANY)
    operands = [in_hbm(blocks), trail if source is None else source, in_hbm(l_rows), in_hbm(mine), in_hbm(theirs)]
    specs = [anywhere, at, pl.BlockSpec((NB, SUP), lambda b: (ahead + b, 0)), anywhere, anywhere]
    if source is not None:
        operands.append(trail)
        specs.append(anywhere)
    scratch = [pltpu.VMEM((SUP, SUP), F32), pltpu.VMEM((NB, 2 * NB), F32), pltpu.VMEM((3, SUP, cols), BF16), pltpu.VMEM((3, NB, SUP), BF16),
               pltpu.VMEM((2, SUP, SUP), F32), pltpu.SemaphoreType.DMA((16,)), pltpu.SemaphoreType.DMA((16,))]
    return call(
        fused_kernel, 100_000_000_000, 1 << 25, 48, grid=(4,),
        out_shape=(near(SUP, SUP), shape(NB, NB), shape(NB, NB), shape(rows, cols)), in_specs=specs, out_specs=(vmem, vmem, vmem, at),
        scratch_shapes=scratch,
        input_output_aliases={1 if source is None else 5: 3},
    )(*operands)


def unpack_kernel(in_ref, rest_ref):
    for n, s in enumerate((3, 2, 1)):
        for half in range(2):
            rest_ref[:, NB * n + LANES * half:NB * n + LANES * half + LANES] = in_ref[pl.ds(4 * half + s, NB, stride=8), :]


def unpack(panel):
    rows = panel.shape[0] - NB
    return call(
        unpack_kernel, 1_000_000, 8 * rows * SUP, 12, grid=(rows // NB,), out_shape=shape(rows, 3 * NB),
        in_specs=[pl.BlockSpec((8 * NB, LANES), lambda i: (i + 1, 0))], out_specs=pl.BlockSpec((NB, 3 * NB), lambda i: (i, 0)),
    )(flat_panel(panel))


def pack_rows(n, cols, diags, out_ref):
    for s in range(4):
        value = jnp.where(n > s, cols[s][...], jnp.where(n == s, diags[s][...], 0.0))
        for half in range(2):
            out_ref[pl.ds(4 * half + s, NB, stride=8), :] = value[:, LANES * half:LANES * half + LANES]


def rows_kernel(*refs):
    (own, y, z, *far), (x_ref, out_ref, own_ref, wide) = refs[:-4], refs[-4:]
    my_col = lax.axis_index("pc")
    i = pl.program_id(0)

    def place(flip, ref):
        wide[:, pl.ds(pl.multiple_of((my_col ^ flip) * NB, NB), NB)] = ref[...]

    place(0, own)
    place(1, y)
    place(2, z)
    if len(far) == 1:
        place(3, far[0])
    else:
        pl.when(i < 2)(lambda: place(3, far[0]))
        pl.when(i >= 2)(lambda: place(3, far[1]))
    for k in range(4):
        lanes = slice(NB * k, NB * k + NB)
        part = dot_nt(wide[:, lanes], x_ref[NB * k:, lanes])
        out_ref[:, NB * k:] = part if k == 0 else out_ref[:, NB * k:] + part
    own_ref[...] = out_ref[:, pl.ds(pl.multiple_of(my_col * NB, NB), NB)]


def solve_rows(pieces, x):
    own, y, z, *far = pieces
    rows = own.shape[0]
    tile = rows // 4
    block = pl.BlockSpec((tile, NB), lambda i: (i, 0))
    far_blocks = [block] if len(far) == 1 else [
        pl.BlockSpec((tile, NB), lambda i: (jnp.minimum(i, 1), 0)), pl.BlockSpec((tile, NB), lambda i: (jnp.maximum(i - 2, 0), 0))]
    return call(
        rows_kernel, 30 * rows * SUP * SUP // 4, 12 * rows * SUP, 34, grid=(4,),
        out_shape=(shape(rows, SUP), shape(rows, NB)),
        in_specs=[block] * 3 + far_blocks + [fixed(SUP, SUP)],
        out_specs=(pl.BlockSpec((tile, SUP), lambda i: (i, 0)), block),
        scratch_shapes=[pltpu.VMEM((tile, SUP), F32)],
    )(in_hbm(own), y, z, *far, x)


def cols_kernel(*refs):
    pieces, x_ref, outs, tall, done = refs[:4], refs[4], refs[5:-2], refs[-2], refs[-1]
    my_row = lax.axis_index("pr")
    i = pl.program_id(0)
    for j in range(4):
        tall[pl.ds(pl.multiple_of((my_row ^ j) * NB, NB), NB), :] = pieces[j][...]

    for k in range(4):
        at = slice(NB * k, NB * k + NB)
        part = dot(x_ref[NB * k:, at], tall[at, :])
        done[NB * k:, :] = part if k == 0 else done[NB * k:, :] + part

    def put(ref):
        ref[...] = done[...]

    if len(outs) == 1:
        put(outs[0])
    else:
        pl.when(i < 4)(lambda: put(outs[0]))
        pl.when(i >= 4)(lambda: put(outs[1]))


def solve_cols(pieces, x):
    cols = pieces[0].shape[1]
    outs = [shape(SUP, min(SUP, cols))] + ([near(SUP, cols - SUP)] if cols > SUP else [])
    specs = [pl.BlockSpec((SUP, NB), lambda i: (0, jnp.minimum(i, min(SUP, cols) // NB - 1))), pl.BlockSpec((SUP, NB), lambda i: (0, jnp.maximum(i - 4, 0)))]
    return call(
        cols_kernel, 30 * cols * SUP * SUP // 4, 12 * cols * SUP, 20, grid=(cols // NB,), out_shape=outs,
        in_specs=[pl.BlockSpec((NB, NB), lambda i: (0, i))] * 4 + [fixed(SUP, SUP)],
        out_specs=specs[:len(outs)], scratch_shapes=[pltpu.VMEM((SUP, NB), F32), pltpu.VMEM((SUP, NB), F32)],
    )(*pieces, x)


def panel_kernel(*refs):
    rest_ref, l_ref, u_ref, diag_ref, col_ref = refs[:5]
    l_parts, u_parts = refs[-2:]
    keep = rest_ref.shape[1] - NB
    i = pl.program_id(0)

    @pl.when(i == 0)
    def _():
        def split_rows(k, carry):
            at = pl.ds(pl.multiple_of(k * 64, 64), 64)
            for n, part in enumerate(split3(u_ref[at, :])):
                u_parts[n, at, :] = part
            return carry

        lax.fori_loop(0, SUP // 64, split_rows, 0)

    for n, part in enumerate(split3(l_ref[...])):
        l_parts[n] = part
    new = rest_ref[...] - dot_parts(lambda n: l_parts[n], lambda n: u_parts[n])

    @pl.when(i == 0)
    def _():
        diag_ref[...] = new[:, keep:]
        if keep:
            refs[5][...] = new[:, :keep]

    @pl.when(i > 0)
    def _():
        col_ref[...] = new[:, keep:]
        if keep:
            refs[6][...] = new[:, :keep]


def update_panel(rest, l_rows, u_panel):
    rows, width = rest.shape
    keep = width - NB
    below = lambda i: (jnp.maximum(i - 1, 0), 0)
    outs = [shape(NB, NB), shape(rows - NB, NB)] + ([shape(NB, keep), shape(rows - NB, keep)] if keep else [])
    specs = [fixed(NB, NB), pl.BlockSpec((NB, NB), below)]
    if keep:
        specs += [fixed(NB, keep), pl.BlockSpec((NB, keep), below)]
    return call(
        panel_kernel, 12 * rows * width * SUP, 8 * rows * width + 4 * rows * SUP, 26, grid=(rows // NB,), out_shape=outs,
        in_specs=[pl.BlockSpec((NB, width), lambda i: (i, 0)), pl.BlockSpec((NB, SUP), lambda i: (i, 0)), fixed(SUP, width)],
        out_specs=specs, scratch_shapes=[pltpu.VMEM((3, NB, SUP), BF16), pltpu.VMEM((3, SUP, width), BF16)],
    )(in_hbm(rest), in_hbm(l_rows), u_panel)


def row_kernel(*refs):
    trail_ref, l_ref, mine_ref, theirs_ref = refs[1:5]
    keep_ref, send_ref = refs[-2:]
    j = pl.program_id(0)
    lanes = pl.ds(pl.multiple_of(j % 2 * (SUP // 2), SUP // 2), SUP // 2)

    @pl.when(j < 2)
    def _():
        keep_ref[:, lanes] = trail_ref[...] - dot(l_ref[...], mine_ref[...])
        if len(refs) == 8:
            keep_ref[:, SUP:] = refs[5][...]
            send_ref[:, SUP:] = refs[5][...]

    @pl.when(j >= 2)
    def _():
        send_ref[:, lanes] = trail_ref[...] - dot(l_ref[...], theirs_ref[...])


def update_row(core, trail, l_rows, mine, theirs, panel_row, step):
    extra = [] if panel_row is None else [panel_row]
    width = SUP + (0 if panel_row is None else panel_row.shape[1])
    out = fixed(NB, width)
    return call(
        row_kernel, 24 * NB * SUP * SUP, 12 * SUP * SUP, 30,
        grid_spec=pltpu.PrefetchScalarGridSpec(
            num_scalar_prefetch=1, grid=(4,),
            in_specs=[pl.BlockSpec((NB, SUP // 2), lambda j, h: (step + 1, 2 * (h[0] ^ (j // 2)) + j % 2)), fixed(NB, SUP),
                      pl.BlockSpec((SUP, SUP // 2), lambda j, h: (0, jnp.minimum(j, 1))), pl.BlockSpec((SUP, SUP // 2), lambda j, h: (0, jnp.maximum(j - 2, 0)))]
            + [fixed(*a.shape) for a in extra],
            out_specs=(out, out)),
        out_shape=(shape(NB, width), shape(NB, width)),
    )(core, trail, in_hbm(l_rows), in_hbm(mine), in_hbm(theirs), *extra)


def trail_kernel(core_ref, trail_ref, l_ref, mine_ref, theirs_ref, diag_ref, *rest):
    rest, (landing, u_parts, l_parts, sem) = rest[:-4], rest[-4:]
    my_row = lax.axis_index("pr")
    j, i = pl.program_id(0), pl.program_id(1)
    quarter = SUP // 4
    first = [pltpu.make_async_copy(mine_ref.at[at], landing.at[at], sem.at[n]) for n, at in enumerate(pl.ds(n * quarter, quarter) for n in range(4))]
    second = pltpu.make_async_copy(theirs_ref, landing, sem.at[4])
    out_ref = rest[8] if len(rest) > 1 else rest[0]

    @pl.when(i == 0)
    def _():
        for copy in first:
            pl.when(j == 0)(copy.start)
        pl.when(j == 1)(second.wait)
        for n, copy in enumerate(first):
            pl.when(j == 0)(copy.wait)

            def split_rows(k, carry, n=n):
                at = pl.ds(pl.multiple_of(n * quarter + k * 64, 64), 64)
                for m, part in enumerate(split3(landing[at, :])):
                    u_parts[m, at, :] = part
                return carry

            lax.fori_loop(0, quarter // 64, split_rows, 0)
        out_ref[...] = dot_tn(diag_ref[...], landing[pl.ds(pl.multiple_of(my_row * NB, NB), NB), :])

    @pl.when(i > 0)
    def _():
        pl.when((i == 1) & (j == 0))(second.start)
        for n, part in enumerate(split3(l_ref[...])):
            l_parts[n] = part
        out_ref[...] = trail_ref[...] - dot_parts(lambda n: l_parts[n], lambda n: u_parts[n])
        if len(rest) > 1:
            count = pl.num_programs(1)
            pack_rows(jnp.minimum(j * (count - 1) + i - 1, count + 2), rest[:4], rest[4:8], rest[9])


def update_trail(core, trail, l_rows, mine, theirs, own_diag, step, out_cols=(), out_diags=()):
    rows, cols = trail.shape
    off = 1 if step < 3 else 0
    count = rows // NB - step - off - (4 if step < 3 else 0)
    at = pl.BlockSpec((NB, SUP), lambda j, i, h: (jnp.where(i == 0, step, step + off + i), h[0] ^ j))
    anywhere = pl.BlockSpec(memory_space=pl.ANY)
    ins = [at, pl.BlockSpec((NB, SUP), lambda j, i, h: (jnp.maximum(i, 1) - 1 + off, 0)), anywhere, anywhere,
           fixed(NB, NB)]
    outs, shapes = [at], [shape(rows, cols)]
    if out_cols:
        block = lambda j, i: jnp.clip(j * (count - 1) + i - 1, 0, rows // NB - 1)
        ins += [pl.BlockSpec((NB, NB), lambda j, i, h, s=s: (jnp.maximum(block(j, i) - s - 1, 0), 0)) for s in range(4)]
        ins += [fixed(NB, NB)] * 4
        outs.append(pl.BlockSpec((8 * NB, LANES), lambda j, i, h: (block(j, i), 0)))
        shapes.append(shape(rows * 8, LANES))
    return call(
        trail_kernel, 12 * count * NB * cols * SUP, 8 * count * NB * cols, 32,
        grid_spec=pltpu.PrefetchScalarGridSpec(num_scalar_prefetch=1, grid=(2, count), in_specs=ins, out_specs=outs, scratch_shapes=[
            pltpu.VMEM((SUP, SUP), F32), pltpu.VMEM((3, SUP, SUP), BF16), pltpu.VMEM((3, NB, SUP), BF16), pltpu.SemaphoreType.DMA((5,))]),
        out_shape=shapes, input_output_aliases={1: 0} if step else {},
    )(core, trail, in_hbm(l_rows), in_hbm(mine), in_hbm(theirs), *(in_hbm(a) for a in (own_diag, *out_cols, *out_diags)))


FLIP1 = [(0, 1), (1, 0), (2, 3), (3, 2)]
FLIP2 = [(0, 2), (2, 0), (1, 3), (3, 1)]
FLIP3 = [(0, 3), (3, 0), (1, 2), (2, 1)]


def gather_diag(block):
    y = functools.partial(lax.ppermute, axis_name="pc", perm=FLIP1)
    z = functools.partial(lax.ppermute, axis_name="pc", perm=FLIP2)
    x = functools.partial(lax.ppermute, axis_name="pr", perm=FLIP2)
    at_y, at_z, at_x = y(block), z(block), x(block)
    at_yz, at_xy, at_xz = z(at_y), x(at_y), x(at_z)
    at_xyz = x(at_yz)
    have = jnp.stack([block, at_y, at_z, at_yz, at_x, at_xy, at_xz, at_xyz])
    return [have, lax.ppermute(have, "pr", FLIP1)]


def gather_cols(keep, send):
    return [keep, lax.ppermute(send, "pr", FLIP1), lax.ppermute(keep, "pr", FLIP2), lax.ppermute(send, "pr", FLIP3)]


def gather_all(panel):
    x = lax.ppermute(panel, "pr", FLIP2)
    other = lax.ppermute(panel, "pr", FLIP1)
    return [panel, other, x, lax.ppermute(x, "pr", FLIP1)]


def solution(mesh):
    def local_part(panel_tile, trail_tile):
        my_row = lax.axis_index("pr")
        half = my_row % 2
        core = jnp.full((1,), half, jnp.int32)
        trail = trail_tile
        out_cols, out_diags = [], []
        for step in range(4):
            if step == 0:
                diag_block, later = lax.optimization_barrier((panel_tile[:NB, 0, :], panel_tile[:NB]))
                blocks = gather_diag(diag_block)
                col_panel = panel_tile[NB:, 0, :]
                keep, send = (lax.dynamic_slice(trail_tile, (0, SUP * h), (NB, SUP)) for h in (half, 1 - half))
                panel_row = jnp.concatenate([later[:NB, s, :] for s in (3, 2, 1)], axis=1)
                rest = unpack(panel_tile)
            else:
                blocks = [lax.all_gather(diag_block, ("pc", "pr"))]
            y = lax.ppermute(col_panel, "pc", FLIP1)
            z = lax.ppermute(col_panel, "pc", FLIP2)
            col_pieces = gather_cols(keep, send)
            if step == 0:
                row_pieces = gather_all(panel_row)
            if step:
                source = trail if step == 1 else None
                trail, = update_trail(core, trail, l_rows, mine, theirs, own_diag, step - 1)
                blocks, trail = lax.optimization_barrier((blocks, trail))
            if step:
                far = [lax.ppermute(col_panel, "pc", FLIP3)]
            else:
                split = col_panel.shape[0] // 2
                far = [lax.ppermute(z[:split], "pc", FLIP1), lax.ppermute(y[split:], "pc", FLIP2)]
            if step == 0:
                x_sup, own_l, own_diag = factor(blocks)
            else:
                x_sup, own_l, own_diag, trail = factor_beside(*blocks, source, trail, l_rows, mine, theirs)
            mine, *more = solve_cols(col_pieces, x_sup)
            if step == 0:
                more = solve_cols(row_pieces, x_sup)
            theirs = lax.ppermute(mine, "pr", FLIP1)
            l_rows, own_col = solve_rows([col_panel, y, z, *far], x_sup)
            out_cols.append(own_col)
            out_diags.append(own_l)
            if step < 3:
                diag_block, col_panel, *left = update_panel(rest, l_rows, more[0])
                panel_row, rest = left if left else (None, None)
                keep, send = update_row(core, trail, l_rows, mine, theirs, panel_row, step)
        trail, flat = update_trail(core, trail, l_rows, mine, theirs, own_diag, 3, out_cols, out_diags)
        rows = trail.shape[0]
        return flat.reshape(rows, 2, 4, LANES).transpose(0, 2, 1, 3).reshape(rows, 4, NB), trail

    spec_panel = P("pr", "pc", None)
    spec_trail = P("pr", "pc")
    return jax.shard_map(local_part, mesh=mesh, in_specs=(spec_panel, spec_trail), out_specs=(spec_panel, spec_trail), check_vma=False)
```

```python
import functools

import jax
import jax.numpy as jnp
from jax import lax
from jax.experimental import pallas as pl
from jax.experimental.pallas import tpu as pltpu
from jax.sharding import PartitionSpec as P


F32 = jnp.float32
BF16 = jnp.bfloat16
HIGH = lax.Precision.HIGHEST
NB = 256
LANES = 128
SUP = 1024
MIB = 1024 * 1024


def dot(a, b):
    return lax.dot_general(a, b, (((1,), (0,)), ((), ())), precision=HIGH, preferred_element_type=F32)


def dot_nt(a, b):
    return lax.dot_general(a, b, (((1,), (1,)), ((), ())), precision=HIGH, preferred_element_type=F32)


def dot_tn(a, b):
    return lax.dot_general(a, b, (((0,), (0,)), ((), ())), precision=HIGH, preferred_element_type=F32)


def split3(x):
    high = x.astype(BF16)
    rest = x - high.astype(F32)
    mid = rest.astype(BF16)
    return high, mid, (rest - mid.astype(F32)).astype(BF16)


def panel32(work, p, filler=lambda: None):
    r0 = 32 * p
    diag_tile = p // 4
    lane0 = r0 % LANES
    tiles = [0, 1, 2] if p < 4 else [1, 2, 3]
    rows = {ti: [work[r0 + 8 * sg:r0 + 8 * sg + 8, LANES * ti:LANES * ti + LANES] for sg in range(4)] for ti in tiles}
    sub_id = lax.broadcasted_iota(jnp.int32, (8, LANES), 0)

    def over_lanes(u, sg):
        return jnp.broadcast_to(rows[diag_tile][sg][:, lane0 + u:lane0 + u + 1], (8, LANES))

    def over_sublanes(v, i):
        return jnp.broadcast_to(v[i:i + 1, :], (8, LANES))

    col, fac = {}, {}
    for u in range(16):
        for sg in range(u // 8, 4):
            col[u, sg] = over_lanes(u, sg)
    filler()
    for g in range(4):
        for t in range(8 * g, 8 * g + 8):
            tt = t - 8 * g
            rs = lax.rsqrt(over_sublanes(col[t, g], tt))
            for sg in range(g, 4):
                fac[t, sg] = col[t, sg] * rs
            for u in range(t + 1, min(8 * g + 16, 32)):
                ug = u // 8
                s = over_sublanes(col[t, ug], u - 8 * ug) * rs if u == t + 1 else over_sublanes(fac[t, ug], u - 8 * ug)
                for sg in range(ug, 4):
                    col[u, sg] = col[u, sg] - fac[t, sg] * s
            for ti in tiles:
                row = over_sublanes(rows[ti][g], tt) * rs
                own = rows[ti][g] - fac[t, g] * row
                rows[ti][g] = jnp.where(sub_id > tt, own, jnp.where(sub_id == tt, row, rows[ti][g]))
                for sg in range(g + 1, 4):
                    rows[ti][sg] = rows[ti][sg] - fac[t, sg] * row
        if g < 2:
            for u in range(8 * g + 16, 8 * g + 24):
                for sg in range(u // 8, 4):
                    col[u, sg] = over_lanes(u, sg)
    for ti in tiles:
        for sg in range(4):
            work[r0 + 8 * sg:r0 + 8 * sg + 8, LANES * ti:LANES * ti + LANES] = rows[ti][sg]
    if p == 7:
        return
    high, mid, low = split3(jnp.concatenate([jnp.concatenate(rows[ti], axis=0) for ti in tiles], axis=1))
    first = (r0 + 32 - LANES * diag_tile) // LANES * LANES
    rhs = jnp.concatenate([high, mid, high, mid, low, high], axis=0)
    lhs = jnp.concatenate([high, high, mid, mid, high, low], axis=0)[:, first:256 - LANES * diag_tile]
    upd = lax.dot_general(lhs, rhs, (((0,), (0,)), ((), ())), preferred_element_type=F32)
    skip = r0 + 32 - first - LANES * diag_tile
    for j, ti in enumerate(tiles):
        lanes = slice(LANES * ti, LANES * ti + LANES)
        work[r0 + 32:256, lanes] = work[r0 + 32:256, lanes] - upd[skip:, LANES * j:LANES * j + LANES]


def spread_factor(b, u_ref, x_ref, work):
    row = lax.broadcasted_iota(jnp.int32, (NB, NB), 0)
    col = lax.broadcasted_iota(jnp.int32, (NB, NB), 1)
    a, e = NB * b, NB * b + NB
    xbb = jnp.where(col <= row, work[:, NB:], 0.0)
    u_ref[a:e, a:e] = jnp.where(col >= row, work[:, :NB], 0.0)
    if b > 0:
        x_ref[a:e, :a] = dot(xbb, x_ref[a:e, :a])
        u_ref[a:e, :a] = jnp.zeros((NB, a), F32)
    x_ref[a:e, a:e] = xbb
    if b < 3:
        urow = dot(xbb, u_ref[a:e, e:])
        u_ref[a:e, e:] = urow
        for c in range(b + 1, 4):
            lo = NB * c
            uc = urow[:, lo - e:lo - e + NB]
            u_ref[lo:lo + NB, lo:] = u_ref[lo:lo + NB, lo:] - dot_tn(uc, urow[:, lo - e:])
            x_ref[lo:lo + NB, :e] = x_ref[lo:lo + NB, :e] - dot_tn(uc, x_ref[a:e, :e])


def factor_block(b, u_ref, x_ref, own_l_ref, own_diag_ref, work, filler=lambda p: None):
    row = lax.broadcasted_iota(jnp.int32, (NB, NB), 0)
    col = lax.broadcasted_iota(jnp.int32, (NB, NB), 1)
    at = pl.ds(pl.multiple_of(b * NB, NB), NB)
    work[:, :NB] = u_ref[at, at]
    work[:, NB:] = jnp.where(row == col, 1.0, 0.0)
    for p in range(8):
        panel32(work, p, functools.partial(filler, p))
    for n in range(4):
        pl.when(b == n)(lambda n=n: spread_factor(n, u_ref, x_ref, work))

    @pl.when(b == 3)
    def _():
        at_row, at_col = (pl.ds(pl.multiple_of(lax.axis_index(name) * NB, NB), NB) for name in ("pr", "pc"))
        own_l_ref[...] = u_ref[at_col, at_row].T
        own_diag_ref[...] = u_ref[at_row, at_row]


def factor_kernel(*refs):
    blocks, (x_ref, own_l_ref, own_diag_ref, u_ref, work) = refs[:-5], refs[-5:]
    my_col, my_row = lax.axis_index("pc"), lax.axis_index("pr")
    b = pl.program_id(0)

    @pl.when(b == 0)
    def _():
        for c in range(4):
            for r in range(4):
                at_row, at_col = (pl.ds(pl.multiple_of(v * NB, NB), NB) for v in (my_row ^ r, my_col ^ c))
                u_ref[at_row, at_col] = blocks[r % 2][c + 4 * (r // 2)]
        x_ref[...] = jnp.zeros_like(x_ref)

    factor_block(b, u_ref, x_ref, own_l_ref, own_diag_ref, work)


def call(kernel, flops, moved, vmem, **kw):
    cost = pl.CostEstimate(flops=flops, bytes_accessed=moved, transcendentals=0)
    return pl.pallas_call(kernel, cost_estimate=cost, compiler_params=pltpu.CompilerParams(vmem_limit_bytes=vmem * MIB), **kw)


def fixed(*dims):
    return pl.BlockSpec(dims, lambda *ids: (0,) * len(dims))


def in_hbm(x):
    return pltpu.with_memory_space_constraint(x, pltpu.HBM)


def shape(*dims):
    return pltpu.HBM(dims, F32)


def near(*dims):
    return jax.ShapeDtypeStruct(dims, F32)


def factor(blocks):
    vmem = pl.BlockSpec(memory_space=pltpu.VMEM)
    return call(
        factor_kernel, 30_000_000_000, 1 << 24, 20, grid=(4,),
        out_shape=(near(SUP, SUP), shape(NB, NB), shape(NB, NB)), in_specs=[vmem] * len(blocks), out_specs=(vmem,) * 3,
        scratch_shapes=[pltpu.VMEM((SUP, SUP), F32), pltpu.VMEM((NB, 2 * NB), F32)],
    )(*blocks)


def flat_panel(panel):
    return panel.reshape(-1, 4, 2, LANES).transpose(0, 2, 1, 3).reshape(-1, LANES)


def dot_parts(a, b):
    total = None
    for i, j in ((2, 0), (0, 2), (1, 1), (1, 0), (0, 1), (0, 0)):
        product = lax.dot_general(a(i), b(j), (((1,), (0,)), ((), ())), preferred_element_type=F32)
        total = product if total is None else total + product
    return total


def fused_kernel(s_ref, trail_ref, l_ref, mine_ref, theirs_ref, *rest):
    x_ref, own_l_ref, own_diag_ref, out_ref, u_ref, work, u_parts, l_parts, landing, block_sem, land_sem = rest[-11:]
    b = pl.program_id(0)
    my_row = lax.axis_index("pr")

    def landing_copy(k, w):
        at = pl.ds(LANES * k, LANES)
        return pltpu.make_async_copy((mine_ref, theirs_ref)[w].at[at], landing.at[w, at], land_sem.at[2 * k + w])

    def block_copy(n):
        return pltpu.make_async_copy(s_ref.at[n], u_ref.at[pl.ds(n % 4 * NB, NB), pl.ds(n // 4 * NB, NB)], block_sem.at[n])

    @pl.when(b == 0)
    def _():
        half = my_row % 2
        for k in range(8):
            for w in range(2):
                landing_copy(k, w).start()
        for n in range(16):
            block_copy(n).start()
        x_ref[...] = jnp.zeros_like(x_ref)
        for k in range(8):
            for w in range(2):
                landing_copy(k, w).wait()

                def split_rows(i, carry, k=k, w=w):
                    at = pl.ds(pl.multiple_of(LANES * k + 32 * i, 32), 32)
                    for n, part in enumerate(split3(landing[w, at, :])):
                        u_parts[n, at, pl.ds(pl.multiple_of((half ^ w) * SUP, SUP), SUP)] = part
                    return carry

                lax.fori_loop(0, 4, split_rows, 0)
        for n in range(16):
            block_copy(n).wait()

    for n, part in enumerate(split3(l_ref[...])):
        l_parts[n] = part

    def beside(q):
        lanes = slice(NB * q, NB * q + NB)
        for k in range(4):
            deep = slice(NB * k, NB * k + NB)
            total = dot_parts(lambda i: l_parts[i, :, deep], lambda j: u_parts[j, deep, lanes])
            out_ref[:, lanes] = (trail_ref if k == 0 else out_ref)[:, lanes] - total

    factor_block(b, u_ref, x_ref, own_l_ref, own_diag_ref, work, beside)


def factor_beside(blocks, source, trail, l_rows, mine, theirs):
    rows, cols = trail.shape
    last = rows // NB - 4
    ahead = l_rows.shape[0] // NB - 4
    vmem = pl.BlockSpec(memory_space=pltpu.VMEM)
    at = pl.BlockSpec((NB, cols), lambda b: (last + b, 0))
    anywhere = pl.BlockSpec(memory_space=pl.ANY)
    operands = [in_hbm(blocks), trail if source is None else source, in_hbm(l_rows), in_hbm(mine), in_hbm(theirs)]
    specs = [anywhere, at, pl.BlockSpec((NB, SUP), lambda b: (ahead + b, 0)), anywhere, anywhere]
    if source is not None:
        operands.append(trail)
        specs.append(anywhere)
    scratch = [pltpu.VMEM((SUP, SUP), F32), pltpu.VMEM((NB, 2 * NB), F32), pltpu.VMEM((3, SUP, cols), BF16), pltpu.VMEM((3, NB, SUP), BF16),
               pltpu.VMEM((2, SUP, SUP), F32), pltpu.SemaphoreType.DMA((16,)), pltpu.SemaphoreType.DMA((16,))]
    return call(
        fused_kernel, 100_000_000_000, 1 << 25, 48, grid=(4,),
        out_shape=(near(SUP, SUP), shape(NB, NB), shape(NB, NB), shape(rows, cols)), in_specs=specs, out_specs=(vmem, vmem, vmem, at),
        scratch_shapes=scratch,
        input_output_aliases={1 if source is None else 5: 3},
    )(*operands)


def unpack_kernel(in_ref, rest_ref):
    for n, s in enumerate((3, 2, 1)):
        for half in range(2):
            rest_ref[:, NB * n + LANES * half:NB * n + LANES * half + LANES] = in_ref[pl.ds(4 * half + s, NB, stride=8), :]


def unpack(panel):
    rows = panel.shape[0] - NB
    return call(
        unpack_kernel, 1_000_000, 8 * rows * SUP, 12, grid=(rows // NB,), out_shape=shape(rows, 3 * NB),
        in_specs=[pl.BlockSpec((8 * NB, LANES), lambda i: (i + 1, 0))], out_specs=pl.BlockSpec((NB, 3 * NB), lambda i: (i, 0)),
    )(flat_panel(panel))


def pack_rows(n, cols, diags, out_ref):
    for s in range(4):
        value = jnp.where(n > s, cols[s][...], jnp.where(n == s, diags[s][...], 0.0))
        for half in range(2):
            out_ref[pl.ds(4 * half + s, NB, stride=8), :] = value[:, LANES * half:LANES * half + LANES]


def rows_kernel(*refs):
    (own, y, z, *far), (x_ref, *_, out_ref, own_ref, wide) = refs[:ROW_PIECES[len(refs)]], refs[ROW_PIECES[len(refs)]:]
    my_col = lax.axis_index("pc")
    i = pl.program_id(0)

    def place(flip, ref):
        wide[:, pl.ds(pl.multiple_of((my_col ^ flip) * NB, NB), NB)] = ref[...]

    place(0, own)
    place(1, y)
    place(2, z)
    if len(far) == 1:
        place(3, far[0])
    else:
        pl.when(i == 0)(lambda: place(3, far[0]))
        pl.when(i > 0)(lambda: place(3, far[1]))
    for k in range(4):
        lanes = slice(NB * k, NB * k + NB)
        part = dot_nt(wide[:, lanes], x_ref[NB * k:, lanes])
        out_ref[:, NB * k:] = part if k == 0 else out_ref[:, NB * k:] + part
    own_ref[...] = out_ref[:, pl.ds(pl.multiple_of(my_col * NB, NB), NB)]


ROW_PIECES = {8: 4, 9: 5, 11: 5}


def solve_rows(pieces, x, part=0, before=()):
    own, y, z, *far = pieces
    rows = own.shape[0]
    tile = rows // 4
    whole = len(far) == 1
    at = (lambda i: (i, 0)) if whole else (lambda i: (2 * i + part, 0))
    block, wide_block = pl.BlockSpec((tile, NB), at), pl.BlockSpec((tile, SUP), at)
    count = 4 if whole else 2
    return call(
        rows_kernel, 30 * count * tile * SUP * SUP // 4, 12 * count * tile * SUP, 34, grid=(count,),
        out_shape=(shape(rows, SUP), shape(rows, NB)),
        in_specs=[block] * 3 + ([block] if whole else [fixed(tile, NB)] * 2) + [fixed(SUP, SUP)] + [pl.BlockSpec(memory_space=pl.ANY)] * len(before),
        out_specs=(wide_block, block), scratch_shapes=[pltpu.VMEM((tile, SUP), F32)],
        input_output_aliases={6: 0, 7: 1} if before else {},
    )(in_hbm(own), y, z, *far, x, *(in_hbm(a) for a in before))


def cols_kernel(*refs):
    pieces, x_ref, outs, tall, done = refs[:4], refs[4], refs[5:-2], refs[-2], refs[-1]
    my_row = lax.axis_index("pr")
    i = pl.program_id(0)
    for j in range(4):
        tall[pl.ds(pl.multiple_of((my_row ^ j) * NB, NB), NB), :] = pieces[j][...]

    for k in range(4):
        at = slice(NB * k, NB * k + NB)
        part = dot(x_ref[NB * k:, at], tall[at, :])
        done[NB * k:, :] = part if k == 0 else done[NB * k:, :] + part

    def put(ref):
        ref[...] = done[...]

    if len(outs) == 1:
        put(outs[0])
    else:
        pl.when(i < 4)(lambda: put(outs[0]))
        pl.when(i >= 4)(lambda: put(outs[1]))


def solve_cols(pieces, x):
    cols = pieces[0].shape[1]
    outs = [shape(SUP, min(SUP, cols))] + ([near(SUP, cols - SUP)] if cols > SUP else [])
    specs = [pl.BlockSpec((SUP, NB), lambda i: (0, jnp.minimum(i, min(SUP, cols) // NB - 1))), pl.BlockSpec((SUP, NB), lambda i: (0, jnp.maximum(i - 4, 0)))]
    return call(
        cols_kernel, 30 * cols * SUP * SUP // 4, 12 * cols * SUP, 20, grid=(cols // NB,), out_shape=outs,
        in_specs=[pl.BlockSpec((NB, NB), lambda i: (0, i))] * 4 + [fixed(SUP, SUP)],
        out_specs=specs[:len(outs)], scratch_shapes=[pltpu.VMEM((SUP, NB), F32), pltpu.VMEM((SUP, NB), F32)],
    )(*pieces, x)


def panel_kernel(*refs):
    rest_ref, l_ref, u_ref, diag_ref, col_ref = refs[:5]
    l_parts, u_parts = refs[-2:]
    keep = rest_ref.shape[1] - NB
    i = pl.program_id(0)

    @pl.when(i == 0)
    def _():
        def split_rows(k, carry):
            at = pl.ds(pl.multiple_of(k * 64, 64), 64)
            for n, part in enumerate(split3(u_ref[at, :])):
                u_parts[n, at, :] = part
            return carry

        lax.fori_loop(0, SUP // 64, split_rows, 0)

    for n, part in enumerate(split3(l_ref[...])):
        l_parts[n] = part
    new = rest_ref[...] - dot_parts(lambda n: l_parts[n], lambda n: u_parts[n])

    @pl.when(i == 0)
    def _():
        diag_ref[...] = new[:, keep:]
        if keep:
            refs[5][...] = new[:, :keep]

    @pl.when(i > 0)
    def _():
        col_ref[...] = new[:, keep:]
        if keep:
            refs[6][...] = new[:, :keep]


def update_panel(rest, l_rows, u_panel):
    rows, width = rest.shape
    keep = width - NB
    below = lambda i: (jnp.maximum(i - 1, 0), 0)
    outs = [shape(NB, NB), shape(rows - NB, NB)] + ([shape(NB, keep), shape(rows - NB, keep)] if keep else [])
    specs = [fixed(NB, NB), pl.BlockSpec((NB, NB), below)]
    if keep:
        specs += [fixed(NB, keep), pl.BlockSpec((NB, keep), below)]
    return call(
        panel_kernel, 12 * rows * width * SUP, 8 * rows * width + 4 * rows * SUP, 26, grid=(rows // NB,), out_shape=outs,
        in_specs=[pl.BlockSpec((NB, width), lambda i: (i, 0)), pl.BlockSpec((NB, SUP), lambda i: (i, 0)), fixed(SUP, width)],
        out_specs=specs, scratch_shapes=[pltpu.VMEM((3, NB, SUP), BF16), pltpu.VMEM((3, SUP, width), BF16)],
    )(in_hbm(rest), in_hbm(l_rows), u_panel)


def row_kernel(*refs):
    trail_ref, l_ref, mine_ref, theirs_ref = refs[1:5]
    keep_ref, send_ref = refs[-2:]
    j = pl.program_id(0)
    lanes = pl.ds(pl.multiple_of(j % 2 * (SUP // 2), SUP // 2), SUP // 2)

    @pl.when(j < 2)
    def _():
        keep_ref[:, lanes] = trail_ref[...] - dot(l_ref[...], mine_ref[...])
        if len(refs) == 8:
            keep_ref[:, SUP:] = refs[5][...]
            send_ref[:, SUP:] = refs[5][...]

    @pl.when(j >= 2)
    def _():
        send_ref[:, lanes] = trail_ref[...] - dot(l_ref[...], theirs_ref[...])


def update_row(core, trail, l_rows, mine, theirs, panel_row, step):
    extra = [] if panel_row is None else [panel_row]
    width = SUP + (0 if panel_row is None else panel_row.shape[1])
    out = fixed(NB, width)
    return call(
        row_kernel, 24 * NB * SUP * SUP, 12 * SUP * SUP, 30,
        grid_spec=pltpu.PrefetchScalarGridSpec(
            num_scalar_prefetch=1, grid=(4,),
            in_specs=[pl.BlockSpec((NB, SUP // 2), lambda j, h: (step + 1, 2 * (h[0] ^ (j // 2)) + j % 2)), fixed(NB, SUP),
                      pl.BlockSpec((SUP, SUP // 2), lambda j, h: (0, jnp.minimum(j, 1))), pl.BlockSpec((SUP, SUP // 2), lambda j, h: (0, jnp.maximum(j - 2, 0)))]
            + [fixed(*a.shape) for a in extra],
            out_specs=(out, out)),
        out_shape=(shape(NB, width), shape(NB, width)),
    )(core, trail, in_hbm(l_rows), in_hbm(mine), in_hbm(theirs), *extra)


def trail_kernel(core_ref, trail_ref, l_ref, mine_ref, theirs_ref, diag_ref, *rest):
    rest, (landing, u_parts, l_parts, sem) = rest[:-4], rest[-4:]
    my_row = lax.axis_index("pr")
    j, i = pl.program_id(0), pl.program_id(1)
    quarter = SUP // 4
    first = [pltpu.make_async_copy(mine_ref.at[at], landing.at[at], sem.at[n]) for n, at in enumerate(pl.ds(n * quarter, quarter) for n in range(4))]
    second = pltpu.make_async_copy(theirs_ref, landing, sem.at[4])
    out_ref = rest[8] if len(rest) > 1 else rest[0]

    @pl.when(i == 0)
    def _():
        for copy in first:
            pl.when(j == 0)(copy.start)
        pl.when(j == 1)(second.wait)
        for n, copy in enumerate(first):
            pl.when(j == 0)(copy.wait)

            def split_rows(k, carry, n=n):
                at = pl.ds(pl.multiple_of(n * quarter + k * 64, 64), 64)
                for m, part in enumerate(split3(landing[at, :])):
                    u_parts[m, at, :] = part
                return carry

            lax.fori_loop(0, quarter // 64, split_rows, 0)
        out_ref[...] = dot_tn(diag_ref[...], landing[pl.ds(pl.multiple_of(my_row * NB, NB), NB), :])

    @pl.when(i > 0)
    def _():
        pl.when((i == 1) & (j == 0))(second.start)
        for n, part in enumerate(split3(l_ref[...])):
            l_parts[n] = part
        out_ref[...] = trail_ref[...] - dot_parts(lambda n: l_parts[n], lambda n: u_parts[n])
        if len(rest) > 1:
            count = pl.num_programs(1)
            pack_rows(jnp.minimum(j * (count - 1) + i - 1, count + 2), rest[:4], rest[4:8], rest[9])


def update_trail(core, trail, l_rows, mine, theirs, own_diag, step, out_cols=(), out_diags=()):
    rows, cols = trail.shape
    off = 1 if step < 3 else 0
    count = rows // NB - step - off - (4 if step < 3 else 0)
    at = pl.BlockSpec((NB, SUP), lambda j, i, h: (jnp.where(i == 0, step, step + off + i), h[0] ^ j))
    anywhere = pl.BlockSpec(memory_space=pl.ANY)
    ins = [at, pl.BlockSpec((NB, SUP), lambda j, i, h: (jnp.maximum(i, 1) - 1 + off, 0)), anywhere, anywhere,
           fixed(NB, NB)]
    outs, shapes = [at], [shape(rows, cols)]
    if out_cols:
        block = lambda j, i: jnp.clip(j * (count - 1) + i - 1, 0, rows // NB - 1)
        ins += [pl.BlockSpec((NB, NB), lambda j, i, h, s=s: (jnp.maximum(block(j, i) - s - 1, 0), 0)) for s in range(4)]
        ins += [fixed(NB, NB)] * 4
        outs.append(pl.BlockSpec((8 * NB, LANES), lambda j, i, h: (block(j, i), 0)))
        shapes.append(shape(rows * 8, LANES))
    return call(
        trail_kernel, 12 * count * NB * cols * SUP, 8 * count * NB * cols, 32,
        grid_spec=pltpu.PrefetchScalarGridSpec(num_scalar_prefetch=1, grid=(2, count), in_specs=ins, out_specs=outs, scratch_shapes=[
            pltpu.VMEM((SUP, SUP), F32), pltpu.VMEM((3, SUP, SUP), BF16), pltpu.VMEM((3, NB, SUP), BF16), pltpu.SemaphoreType.DMA((5,))]),
        out_shape=shapes, input_output_aliases={1: 0} if step else {},
    )(core, trail, in_hbm(l_rows), in_hbm(mine), in_hbm(theirs), *(in_hbm(a) for a in (own_diag, *out_cols, *out_diags)))


FLIP1 = [(0, 1), (1, 0), (2, 3), (3, 2)]
FLIP2 = [(0, 2), (2, 0), (1, 3), (3, 1)]
FLIP3 = [(0, 3), (3, 0), (1, 2), (2, 1)]


def gather_diag(block):
    y = functools.partial(lax.ppermute, axis_name="pc", perm=FLIP1)
    z = functools.partial(lax.ppermute, axis_name="pc", perm=FLIP2)
    x = functools.partial(lax.ppermute, axis_name="pr", perm=FLIP2)
    at_y, at_z, at_x = y(block), z(block), x(block)
    at_yz, at_xy, at_xz = z(at_y), x(at_y), x(at_z)
    at_xyz = x(at_yz)
    have = jnp.stack([block, at_y, at_z, at_yz, at_x, at_xy, at_xz, at_xyz])
    return [have, lax.ppermute(have, "pr", FLIP1)]


def gather_cols(keep, send):
    return [keep, lax.ppermute(send, "pr", FLIP1), lax.ppermute(keep, "pr", FLIP2), lax.ppermute(send, "pr", FLIP3)]


def gather_all(panel):
    x = lax.ppermute(panel, "pr", FLIP2)
    other = lax.ppermute(panel, "pr", FLIP1)
    return [panel, other, x, lax.ppermute(x, "pr", FLIP1)]


def solution(mesh):
    def local_part(panel_tile, trail_tile):
        my_row = lax.axis_index("pr")
        half = my_row % 2
        core = jnp.full((1,), half, jnp.int32)
        trail = trail_tile
        out_cols, out_diags = [], []
        for step in range(4):
            if step == 0:
                diag_block, later = lax.optimization_barrier((panel_tile[:NB, 0, :], panel_tile[:NB]))
                blocks = gather_diag(diag_block)
                col_panel = panel_tile[NB:, 0, :]
                keep, send = (lax.dynamic_slice(trail_tile, (0, SUP * h), (NB, SUP)) for h in (half, 1 - half))
                panel_row = jnp.concatenate([later[:NB, s, :] for s in (3, 2, 1)], axis=1)
                rest = unpack(panel_tile)
            else:
                blocks = [lax.all_gather(diag_block, ("pc", "pr"))]
            y = lax.ppermute(col_panel, "pc", FLIP1)
            z = lax.ppermute(col_panel, "pc", FLIP2)
            col_pieces = gather_cols(keep, send)
            if step == 0:
                row_pieces = gather_all(panel_row)
            if step:
                source = trail if step == 1 else None
                trail, = update_trail(core, trail, l_rows, mine, theirs, own_diag, step - 1)
                blocks, trail = lax.optimization_barrier((blocks, trail))
            if step:
                far = [lax.ppermute(col_panel, "pc", FLIP3)]
            else:
                tile = col_panel.shape[0] // 4
                far = [lax.ppermute(z[:tile], "pc", FLIP1), lax.ppermute(y[2 * tile:3 * tile], "pc", FLIP2)]
                later_far = [lax.ppermute(z[tile:2 * tile], "pc", FLIP1), lax.ppermute(y[3 * tile:], "pc", FLIP2)]
            if step == 0:
                x_sup, own_l, own_diag = factor(blocks)
            else:
                x_sup, own_l, own_diag, trail = factor_beside(*blocks, source, trail, l_rows, mine, theirs)
            mine, *more = solve_cols(col_pieces, x_sup)
            if step == 0:
                more = solve_cols(row_pieces, x_sup)
            theirs = lax.ppermute(mine, "pr", FLIP1)
            l_rows, own_col = solve_rows([col_panel, y, z, *far], x_sup)
            if step == 0:
                l_rows, own_col = solve_rows([col_panel, y, z, *later_far], x_sup, 1, (l_rows, own_col))
            out_cols.append(own_col)
            out_diags.append(own_l)
            if step < 3:
                diag_block, col_panel, *left = update_panel(rest, l_rows, more[0])
                panel_row, rest = left if left else (None, None)
                keep, send = update_row(core, trail, l_rows, mine, theirs, panel_row, step)
        trail, flat = update_trail(core, trail, l_rows, mine, theirs, own_diag, 3, out_cols, out_diags)
        rows = trail.shape[0]
        return flat.reshape(rows, 2, 4, LANES).transpose(0, 2, 1, 3).reshape(rows, 4, NB), trail

    spec_panel = P("pr", "pc", None)
    spec_trail = P("pr", "pc")
    return jax.shard_map(local_part, mesh=mesh, in_specs=(spec_panel, spec_trail), out_specs=(spec_panel, spec_trail), check_vma=False)
```
